128 devices in a mesh: pair: 8 (over x, core), aux: 16 (over y, z).
Axes of the slice: x: 4, y: 4, z: 4, core: 2. Of those that a mesh axis runs over, the one named last changes fastest.
Arguments:
- left_active: bfloat16 [80, 128, 61440], P('pair', None, 'aux'), may hold values from -0.375 to 0.375
- right_active: bfloat16 [80, 128, 61440], P('pair', None, 'aux'), may hold values from -0.375 to 0.375
- amps_active: bfloat16 [80, 128, 128], P('pair', 'aux'), may hold values from -0.5 to 0.5
- rank_active: int32 [80], P('pair'), may hold values from 80 to 128, as said below
- gap_active: float32 [80], P('pair'), may hold values from 0.5 to 2
- energy_active: float32 [80, 128], P('pair'), may hold values from 0.5 to 4
- intersect_active: bfloat16 [80, 4, 128, 128], P('pair'), may hold values from -0.75 to 0.75
- fock_active: float32 [80, 4], P('pair'), may hold values from -2 to 2
- neighbor_active: int32 [80, 4], P('pair'), may hold values from 0 to 79
- left_env: bfloat16 [32, 48, 61440], P('pair', None, 'aux'), may hold values from -0.375 to 0.375
- right_env: bfloat16 [32, 48, 61440], P('pair', None, 'aux'), may hold values from -0.375 to 0.375
- amps_env: bfloat16 [32, 48, 48], P('pair', 'aux'), may hold values from -0.875 to 0.875
- rank_env: int32 [32], P('pair'), may hold values from 24 to 48, as said below
- gap_env: float32 [32], P('pair'), may hold values from 0.5 to 2
- energy_env: float32 [32, 48], P('pair'), may hold values from 0.5 to 4
- intersect_env: bfloat16 [32, 4, 48, 48], P('pair'), may hold values from -1.25 to 1.25
- fock_env: float32 [32, 4], P('pair'), may hold values from -2 to 2
- neighbor_env: int32 [32, 4], P('pair'), may hold values from 0 to 31
Outputs:
- new_active: float32 [80, 128, 128], P('pair', 'aux')
- new_env: float32 [32, 48, 48], P('pair', 'aux')
The draws below stay inside these ranges and needn't reach their ends.
Inputs may be any that keep to these rules, and one draw needn't show every extreme that they name: `rank_active`: multiples of 8; the first active pair has rank 128. `rank_env`: multiples of 8; the first environment pair has rank 48.
All inputs are finite; a program needn't handle non-finite values.
Results may differ from the reference program's by a relative error of at most 0.0041.
Values may be sent and summed in bfloat16 or wider, within the bound.
A program may use at most 128 MiB of HBM per device.

```python
import math
import jax
import jax.numpy as jnp
from jax import lax

RA = 128
RE = 48
NAUX = 61440
NB = 4
PA = 80
PE = 32


def draw_rank_active(key, part):
    values = 8 * jax.random.randint(key, (PA,), RA * 5 // 64, RA // 8 + 1)
    return values.at[0].set(RA).astype(jnp.int32)


def draw_rank_env(key, part):
    values = 8 * jax.random.randint(key, (PE,), RE // 16, RE // 8 + 1)
    return values.at[0].set(RE).astype(jnp.int32)


def set_ends(array, key, least, high):
    longest = array.shape.index(max(array.shape))
    spots = []
    for shift in (0, 1):
        where = [jax.random.randint(jax.random.fold_in(key, axis), (), 0, length) for axis, length in enumerate(array.shape)]
        where[longest] = (where[longest] + shift) % array.shape[longest]
        spots.append(tuple(where))
    return array.at[spots[0]].set(least).at[spots[1]].set(high)


def block_scale(own_key, extent, shards, least, largest):
    factor_of = 1.0
    for position, blocks in shards:
        steps = jax.random.uniform(jax.random.fold_in(jax.random.fold_in(own_key, 6), position), (blocks,), jnp.float32, least / len(shards), largest / len(shards))
        factor_of = factor_of * jnp.repeat(jnp.exp(steps), extent[position] // blocks).reshape((-1,) + (1,) * (len(extent) - 1 - position))
    return factor_of


def normal_values(own_key, dims, width, most, pieces=(), held_as=jnp.bfloat16):
    factor_of = block_scale(own_key, dims, pieces, -0.22, 0.18) if pieces else 1.0
    entries = jax.random.normal(own_key, dims, jnp.float32) * width * factor_of
    return jnp.minimum(jnp.maximum(entries, -most), most).astype(held_as)


def setup_inputs(seed: int = 0) -> dict:
    key_list = jax.random.split(jax.random.key(seed), 19)
    left_active = normal_values(key_list[0], (PA, RA, NAUX), (NAUX ** -0.25), 0.375, ((0, 8), (2, 16)))
    right_active = normal_values(key_list[1], (PA, RA, NAUX), (NAUX ** -0.25), 0.375, ((0, 8), (2, 16)))
    amps_active = normal_values(key_list[2], (PA, RA, RA), (RA ** -0.5), 0.5, ((0, 8), (1, 16)))
    rank_active = draw_rank_active(jax.random.fold_in(key_list[18], 71), 0)
    gap_active = jnp.clip(jnp.exp(math.log(2.0) - 1.3862944 * jax.random.uniform(key_list[4], (PA,), jnp.float32) ** block_scale(key_list[4], (PA,), ((0, 8),), -0.2, 0.2)), 0.5, 2.0)
    energy_active = jnp.clip(jnp.exp(math.log(4.0) - 2.0794415 * jax.random.uniform(key_list[5], (PA, RA), jnp.float32) ** block_scale(key_list[5], (PA, RA), ((0, 8),), -0.2, 0.2)), 0.5, 4.0)
    intersect_active = normal_values(key_list[6], (PA, NB, RA, RA), (RA // 2) ** -0.5, 0.75, ((0, 8),))
    fock_active = jnp.clip(jax.random.uniform(key_list[7], (PA, NB), jnp.float32, -2.0, 2.0) * block_scale(key_list[7], (PA, NB), ((0, 8),), -0.4, 0.0), -2.0, 2.0)
    neighbor_active = set_ends(jax.random.randint(key_list[8], (PA, NB), 0, PA), jax.random.fold_in(key_list[8], 1), 0, PA - 1).astype(jnp.int32)
    left_env = normal_values(key_list[9], (PE, RE, NAUX), (NAUX ** -0.25), 0.375, ((0, 8), (2, 16)))
    right_env = normal_values(key_list[10], (PE, RE, NAUX), (NAUX ** -0.25), 0.375, ((0, 8), (2, 16)))
    amps_env = normal_values(key_list[11], (PE, RE, RE), (RE ** -0.5), 0.875, ((0, 8), (1, 16)))
    rank_env = draw_rank_env(jax.random.fold_in(key_list[18], 71), 0)
    gap_env = jnp.clip(jnp.exp(math.log(2.0) - 1.3862944 * jax.random.uniform(key_list[13], (PE,), jnp.float32) ** block_scale(key_list[13], (PE,), ((0, 8),), -0.2, 0.2)), 0.5, 2.0)
    energy_env = jnp.clip(jnp.exp(math.log(4.0) - 2.0794415 * jax.random.uniform(key_list[14], (PE, RE), jnp.float32) ** block_scale(key_list[14], (PE, RE), ((0, 8),), -0.2, 0.2)), 0.5, 4.0)
    intersect_env = normal_values(key_list[15], (PE, NB, RE, RE), (RE // 2) ** -0.5, 1.25, ((0, 8),))
    fock_env = jnp.clip(jax.random.uniform(key_list[16], (PE, NB), jnp.float32, -2.0, 2.0) * block_scale(key_list[16], (PE, NB), ((0, 8),), -0.4, 0.0), -2.0, 2.0)
    neighbor_env = set_ends(jax.random.randint(key_list[17], (PE, NB), 0, PE), jax.random.fold_in(key_list[17], 1), 0, PE - 1).astype(jnp.int32)
    return dict(left_active=left_active, right_active=right_active, amps_active=amps_active, rank_active=rank_active, gap_active=gap_active, energy_active=energy_active, intersect_active=intersect_active, fock_active=fock_active, neighbor_active=neighbor_active, left_env=left_env, right_env=right_env, amps_env=amps_env, rank_env=rank_env, gap_env=gap_env, energy_env=energy_env, intersect_env=intersect_env, fock_env=fock_env, neighbor_env=neighbor_env)


HIGHEST = lax.Precision.HIGHEST


def rank_masks(pair_ranks, full_width):
    positions = jnp.arange(full_width, dtype=jnp.int32)
    return (positions[None, :, None] < pair_ranks[:, None, None]) & (positions[None, None, :] < pair_ranks[:, None, None])


def update_level(left_ints, right_ints, amplitudes, pair_ranks, pair_gaps, energy, intersect, fock_weights, neighbor, with_ladder):
    full_width = amplitudes.shape[1]
    inside = rank_masks(pair_ranks, full_width)
    masked = jnp.where(inside, amplitudes, jnp.zeros_like(amplitudes))

    def one_pair(pair_items):
        left_pair, right_pair, amp_pair, over_pair, fock_pair, neigh_pair = pair_items
        summed_terms = jnp.dot(left_pair, right_pair.T, preferred_element_type=jnp.float32)
        if with_ladder:
            cross_left = jnp.dot(amp_pair.T, left_pair, preferred_element_type=jnp.float32).astype(jnp.bfloat16)
            cross_right = jnp.dot(amp_pair, right_pair, preferred_element_type=jnp.float32).astype(jnp.bfloat16)
            summed_terms = summed_terms + jnp.dot(cross_left, right_pair.T, preferred_element_type=jnp.float32)
            summed_terms = summed_terms + jnp.dot(cross_left, cross_right.T, preferred_element_type=jnp.float32)
        near_amps = masked[neigh_pair]
        half_product = jnp.einsum('krs,kst->krt', over_pair, near_amps, preferred_element_type=jnp.float32)
        full_product = jnp.einsum('krt,kut->kru', half_product, over_pair.astype(jnp.float32), precision=HIGHEST)
        return summed_terms + jnp.einsum('k,kru->ru', fock_pair, full_product, precision=HIGHEST)

    residual = lax.map(one_pair, (left_ints, right_ints, masked, intersect, fock_weights, neighbor))
    denominator = energy[:, :, None] + energy[:, None, :] + pair_gaps[:, None, None]
    return jnp.where(inside, masked.astype(jnp.float32) - residual / denominator, jnp.float32(0.0))


def reference(left_active, right_active, amps_active, rank_active, gap_active, energy_active, intersect_active, fock_active, neighbor_active, left_env, right_env, amps_env, rank_env, gap_env, energy_env, intersect_env, fock_env, neighbor_env):
    new_active = update_level(left_active, right_active, amps_active, rank_active, gap_active, energy_active, intersect_active, fock_active, neighbor_active, True)
    new_env = update_level(left_env, right_env, amps_env, rank_env, gap_env, energy_env, intersect_env, fock_env, neighbor_env, False)
    return (new_active, new_env)
```

```python
import functools

import jax
import jax.numpy as jnp
from jax import lax
from jax.experimental import pallas as pl
from jax.experimental.pallas import tpu as pltpu
from jax.sharding import PartitionSpec as P

MESH = pl.DeviceIdType.MESH
F32, BF16, I32 = jnp.float32, jnp.bfloat16, jnp.int32
AHEAD = 4
CHUNKS = ((0, 5), (5, 10))


def halves(x):
    high = x.astype(BF16)
    return high, (x - high.astype(F32)).astype(BF16)


def dot(a, b, ca, cb):
    return lax.dot_general(a, b, (((ca,), (cb,)), ((), ())), preferred_element_type=F32)


def iota(shape, dim):
    return lax.broadcasted_iota(I32, shape, dim)


def cat(parts, axis):
    return jnp.concatenate(parts, axis=axis)


def hops(d, n):
    return min(d, n - d)


def kernel(
    npair, ny, nz,
    nbr_a, rank_a, fock_a, gap_a, nbr_e, rank_e, fock_e, gap_e,
    amps_a, en_a, amps_e, en_e,
    la_hbm, ra_hbm, sa_hbm, le_hbm, re_hbm, se_hbm,
    out_a, out_e,
    la, ra, sa, le, re, se,
    gat0, gat1, blk_a, blk_e, tot, bhl, wsel, amp_a, rec_a, amp_e, rec_e,
    send0, send1, recv0, recv1,
    la_sem, ra_sem, le_sem, re_sem, sa_sem, se_sem,
    gat_s, gat_r, blk_s, blk_r, ble_s, ble_r, rs_s, rs_r,
):
    me, grp = lax.axis_index("aux"), lax.axis_index("pair")
    naux = ny * nz
    my, mz = me // nz, lax.rem(me, nz)
    count_a, rows_a, wide_a = amps_a.shape
    rows_e, count_e, wide_e = amps_e.shape
    nb = nbr_a.shape[0]
    lanes = wide_a
    start_a, start_e = me * rows_a, me * rows_e
    gats, sends, recvs = (gat0, gat1), (send0, send1), (recv0, recv1)

    far = sorted(
        ((dy, dz) for dy in range(ny) for dz in range(nz) if dy or dz),
        key=lambda o: -(hops(o[0], ny) + hops(o[1], nz)),
    )

    def peer_of(o):
        return lax.rem(my + o[0], ny) * nz + lax.rem(mz + o[1], nz)

    barrier = pltpu.get_barrier_semaphore()
    for o in far:
        pl.semaphore_signal(barrier, inc=1, device_id={"aux": peer_of(o)}, device_id_type=MESH)
    for d in range(1, npair):
        pl.semaphore_signal(
            barrier, inc=1, device_id={"pair": lax.rem(grp + d, npair)}, device_id_type=MESH
        )

    def load_pair(p):
        return (
            pltpu.make_async_copy(la_hbm.at[p], la.at[p], la_sem.at[p]),
            pltpu.make_async_copy(ra_hbm.at[p], ra.at[p], ra_sem.at[p]),
        )

    load_env = (
        pltpu.make_async_copy(le_hbm, le, le_sem),
        pltpu.make_async_copy(re_hbm, re, re_sem),
    )
    load_se = pltpu.make_async_copy(se_hbm, se, se_sem)
    load_sa = pltpu.make_async_copy(sa_hbm, sa, sa_sem)
    for copy in (load_sa, load_se) + load_env:
        copy.start()
    for p in range(AHEAD):
        for copy in load_pair(p):
            copy.start()

    row8, col8 = iota((rows_a, lanes), 0), iota((rows_a, lanes), 1)
    for p in range(count_a):
        inside = (start_a + row8 < rank_a[p]) & (col8 < rank_a[p])
        own = jnp.where(inside, amps_a[p].astype(F32), 0.0)
        amp_a[p] = own
        own = own.astype(BF16)
        c = 0 if p < CHUNKS[0][1] else 1
        gats[c][me, p - CHUNKS[c][0]] = own
        blk_a[grp * count_a + p] = own

    def own_env(q):
        rows = jnp.zeros((8, wide_e), F32)
        r, s = iota((8, wide_e), 0), iota((8, wide_e), 1)
        for i in range(rows_e):
            rows = jnp.where(r == i, amps_e[i, q : q + 1, :].astype(F32), rows)
        inside = (r < rows_e) & (start_e + r < rank_e[q]) & (s < rank_e[q])
        return jnp.where(inside, rows, 0.0), inside

    owns = [own_env(q) for q in range(count_e)]
    for q in range(count_e):
        at = grp * count_e + q
        blk_e[at] = jnp.zeros(blk_e.shape[1:], BF16)
        blk_e[at, :, :wide_e] = owns[q][0].astype(BF16)

    pl.semaphore_wait(barrier, naux + npair - 2)

    def to_aux(c, o):
        e = o[0] * nz + o[1]
        slot = gats[c].at[me]
        return pltpu.make_async_remote_copy(
            src_ref=slot, dst_ref=slot, send_sem=gat_s.at[c, e], recv_sem=gat_r.at[c, e],
            device_id={"aux": peer_of(o)}, device_id_type=MESH,
        )

    def to_pair(d, block, count, s, r):
        slot = block.at[pl.ds(grp * count, count)]
        return pltpu.make_async_remote_copy(
            src_ref=slot, dst_ref=slot, send_sem=s.at[d], recv_sem=r.at[d],
            device_id={"pair": lax.rem(grp + d, npair)}, device_id_type=MESH,
        )

    for c in range(2):
        for o in far:
            to_aux(c, o).start()
        if c == 0:
            for d in range(1, npair):
                to_pair(d, blk_a, count_a, blk_s, blk_r).start()
                to_pair(d, blk_e, count_e, ble_s, ble_r).start()

    for p in range(count_a):
        inside = (start_a + row8 < rank_a[p]) & (col8 < rank_a[p])
        across = jnp.broadcast_to(en_a[p : p + 1, :], (rows_a, lanes))
        down = jnp.sum(jnp.where(col8 == start_a + row8, across, 0.0), axis=1, keepdims=True)
        rec_a[p] = jnp.where(inside, 1.0 / (across + down + gap_a[p]), 0.0)
    r48, c48 = iota((8, wide_e), 0), iota((8, wide_e), 1)
    for q in range(count_e):
        across = jnp.broadcast_to(en_e[q : q + 1, :], (8, wide_e))
        down = jnp.sum(jnp.where(c48 == start_e + r48, across, 0.0), axis=1, keepdims=True)
        denom = jnp.where(r48 < rows_e, across + down + gap_e[q], 1.0)
        rec_e[q] = jnp.where(owns[q][1], 1.0 / denom, 0.0)
        amp_e[q] = owns[q][0]

    load_sa.wait()
    k_in, k_out = iota((nb * wide_a, lanes), 0), iota((nb * wide_a, lanes), 1)
    group = nb * rows_a
    k_at = lax.rem(k_out, group)
    source = (k_at // rows_a) * wide_a + start_a + lax.rem(k_at, rows_a)
    pick = jnp.where((k_in == source) & (k_out < 2 * group), 1.0, 0.0).astype(BF16)

    def overs(p):
        return cat([sa[p, k] for k in range(nb)], 1)

    @pl.loop(0, count_a)
    def _(p):
        wsel[p] = dot(overs(p), pick, 1, 0).astype(BF16)

    for copy in load_env:
        copy.wait()
    le_all = le[...].reshape(count_e * wide_e, le.shape[2])
    pad = 64 - wide_e
    gap_rows = jnp.zeros((pad, re.shape[2]), BF16)
    re_all = cat([x for q in range(count_e) for x in (re[q], gap_rows)], 0)
    base_e = dot(le_all, re_all, 1, 1)
    low_lanes = iota((wide_e, lanes), 1) < 64
    base_h = []
    for h in range(count_e // 2):
        block = base_e[:, h * lanes : (h + 1) * lanes]
        a, b = 2 * h * wide_e, (2 * h + 1) * wide_e
        base_h.append(jnp.where(low_lanes, block[a : a + wide_e], block[b : b + wide_e]))

    @pl.loop(0, count_a)
    def _(p):
        @pl.when(p + AHEAD < count_a)
        def _():
            for copy in load_pair(p + AHEAD):
                copy.start()

        for copy in load_pair(p):
            copy.wait()
        base = dot(la[p], ra[p], 1, 1)
        tot[p] = base
        bhl[p] = cat(halves(base), 0)

    @pl.loop(1, npair)
    def _(d):
        to_pair(d, blk_a, count_a, blk_s, blk_r).wait()
        to_pair(d, blk_e, count_e, ble_s, ble_r).wait()

    load_se.wait()
    fill = jnp.zeros((pad, wide_e), BF16)
    lane16, row16 = iota((16, lanes), 1), iota((16, lanes), 0)
    keep16 = (lane16 < 64) == (row16 < 8)
    pin, pout = iota((wide_e, lanes), 0), iota((wide_e, lanes), 1)
    pat = lax.rem(pout, 64)
    inner = lax.rem(pat, 8)
    sums = []
    for h in range(count_e // 2):
        q0, q1 = 2 * h, 2 * h + 1
        parts, chosen = [], jnp.zeros((wide_e, lanes), F32)
        for k in range(nb):
            both = cat([se[q0, k], fill, se[q1, k], fill], 0)
            rows = cat(
                [blk_e[nbr_e[q, k], :, :wide_e].astype(F32) for q in (q0, q1)], 0
            ).astype(BF16)
            prod = dot(rows, both, 1, 1)
            scale = jnp.where(row16 < 8, fock_e[q0, k], fock_e[q1, k])
            parts.append(jnp.where(keep16, prod * scale, 0.0))
            for b, q in enumerate((q0, q1)):
                sel = jnp.where(
                    (pin == start_e + inner) & (inner < rows_e) & (pat // 8 == 2 * k + b), 1.0, 0.0
                ).astype(BF16)
                chosen = chosen + dot(se[q, k], sel, 1, 0)
        near = cat(halves(cat(parts, 0)), 0)
        sums.append((base_h[h] + dot(chosen.astype(BF16), near, 1, 0)).astype(BF16))
    both_e = cat(sums, 0)
    srow, scol = iota((lanes, 2 * wide_e), 0), iota((lanes, 2 * wide_e), 1)
    sj, sr = srow // 8, lax.rem(srow, 8)
    si = lax.rem(sr, 4)
    spread = jnp.where(
        (scol == (sr // 4) * wide_e + rows_e * sj + si) & (si < rows_e), 1.0, 0.0
    ).astype(BF16)
    packed = dot(spread, both_e, 1, 0)
    for j in range(naux):
        send1[j, CHUNKS[1][1] - CHUNKS[1][0]] = packed[8 * j : 8 * j + 8].astype(BF16)

    @pl.loop(0, count_a)
    def _(p):
        rows = []
        zero = jnp.zeros((rows_a, wide_a), F32)
        for k in range(nb):
            near = blk_a[nbr_a[k, p]].astype(F32)
            rows.append(cat([near if i == k else zero for i in range(nb)], 1))
        right = dot(cat(rows, 0).astype(BF16), overs(p), 1, 1)
        right = cat(
            [right[k * rows_a : (k + 1) * rows_a] * fock_a[k, p] for k in range(nb)], 0
        )
        tot[p] = tot[p] + dot(wsel[p][:, : 2 * group], cat(halves(right), 0), 1, 0)

    def sums_to(c, o):
        e = o[0] * nz + o[1]
        return pltpu.make_async_remote_copy(
            src_ref=sends[c].at[peer_of(o)], dst_ref=recvs[c].at[e],
            send_sem=rs_s.at[c, e], recv_sem=rs_r.at[c, e],
            device_id={"aux": peer_of(o)}, device_id_type=MESH,
        )

    for c, (lo, hi) in enumerate(CHUNKS):
        for o in far:
            to_aux(c, o).wait()
        for p in range(lo, hi):
            amp = gats[c][:, p - lo].astype(F32).reshape(wide_a, wide_a).astype(BF16)
            x = dot(cat([amp, amp], 0), bhl[p], 0, 0)
            y = dot(cat(halves(x), 1), cat([amp, amp], 1), 1, 1)
            total = (tot[p] + x + y).reshape(naux, rows_a, wide_a)
            sends[c][:, p - lo] = total.astype(BF16)
        for o in far:
            sums_to(c, o).start()

    near_first = far[::-1]
    for c, (lo, hi) in enumerate(CHUNKS):
        acc = sends[c][me].astype(F32)
        for o in near_first:
            sums_to(c, o).wait()
            acc = acc + recvs[c][o[0] * nz + o[1]].astype(F32)
        for p in range(lo, hi):
            out_a[p] = amp_a[p] - acc[p - lo] * rec_a[p]
        if c == 1:
            env = acc[hi - lo]
            turned = pltpu.roll(env, 64, 1)
            for q in range(count_e):
                r = 4 * (q // 2)
                block = (env if q % 2 == 0 else turned)[r : r + 4, :wide_e]
                new = amp_e[q][:4] - block * rec_e[q][:4]
                for i in range(rows_e):
                    out_e[i, q : q + 1, :] = new[i : i + 1]


def shards(
    npair, ny, nz,
    left_active, right_active, amps_active, rank_active, gap_active, energy_active,
    intersect_active, fock_active, neighbor_active,
    left_env, right_env, amps_env, rank_env, gap_env, energy_env,
    intersect_env, fock_env, neighbor_env,
):
    naux = ny * nz
    count_a, rows_a, wide_a = amps_active.shape
    count_e, rows_e, wide_e = amps_env.shape
    nb = neighbor_active.shape[1]
    smem = pl.BlockSpec(memory_space=pltpu.SMEM)
    vmem = pl.BlockSpec(memory_space=pltpu.VMEM)
    anyw = pl.BlockSpec(memory_space=pl.ANY)
    dma = pltpu.SemaphoreType.DMA
    n0 = CHUNKS[0][1] - CHUNKS[0][0]
    n1 = CHUNKS[1][1] - CHUNKS[1][0]
    new_active, new_env = pl.pallas_call(
        functools.partial(kernel, npair, ny, nz),
        out_shape=(
            jax.ShapeDtypeStruct((count_a, rows_a, wide_a), F32),
            jax.ShapeDtypeStruct((rows_e, count_e, wide_e), F32),
        ),
        in_specs=[smem] * 8 + [vmem] * 4 + [anyw] * 6,
        out_specs=(vmem, vmem),
        scratch_shapes=[
            pltpu.VMEM(left_active.shape, BF16),
            pltpu.VMEM(right_active.shape, BF16),
            pltpu.VMEM(intersect_active.shape, BF16),
            pltpu.VMEM(left_env.shape, BF16),
            pltpu.VMEM(right_env.shape, BF16),
            pltpu.VMEM(intersect_env.shape, BF16),
            pltpu.VMEM((naux, n0, rows_a, wide_a), BF16),
            pltpu.VMEM((naux, n1, rows_a, wide_a), BF16),
            pltpu.VMEM((npair * count_a, rows_a, wide_a), BF16),
            pltpu.VMEM((npair * count_e, 8, 128), BF16),
            pltpu.VMEM((count_a, wide_a, wide_a), F32),
            pltpu.VMEM((count_a, 2 * wide_a, wide_a), BF16),
            pltpu.VMEM((count_a, wide_a, 128), BF16),
            pltpu.VMEM((count_a, rows_a, wide_a), F32),
            pltpu.VMEM((count_a, rows_a, wide_a), F32),
            pltpu.VMEM((count_e, 8, wide_e), F32),
            pltpu.VMEM((count_e, 8, wide_e), F32),
            pltpu.VMEM((naux, n0, rows_a, wide_a), BF16),
            pltpu.VMEM((naux, n1 + 1, rows_a, wide_a), BF16),
            pltpu.VMEM((naux, n0, rows_a, wide_a), BF16),
            pltpu.VMEM((naux, n1 + 1, rows_a, wide_a), BF16),
            dma((count_a,)), dma((count_a,)), dma, dma, dma, dma,
            dma((2, naux)), dma((2, naux)),
            dma((npair,)), dma((npair,)), dma((npair,)), dma((npair,)),
            dma((2, naux)), dma((2, naux)),
        ],
        compiler_params=pltpu.CompilerParams(
            collective_id=0, has_side_effects=True, vmem_limit_bytes=60 * 1024 * 1024
        ),
    )(
        neighbor_active.T, rank_active, fock_active.T, gap_active,
        neighbor_env, rank_env, fock_env, gap_env,
        amps_active, energy_active, amps_env.transpose(1, 0, 2), energy_env,
        left_active, right_active, intersect_active, left_env, right_env, intersect_env,
    )
    return new_active, new_env.transpose(1, 0, 2)


def solution(mesh):
    ints, amps = P("pair", None, "aux"), P("pair", "aux", None)
    one, two, four = P("pair"), P("pair", None), P("pair", None, None, None)
    level = (ints, ints, amps, one, one, two, four, two, two)
    naux = mesh.shape["aux"]
    ny = next(n for n in range(int(naux**0.5), 0, -1) if naux % n == 0)
    return jax.shard_map(
        functools.partial(shards, mesh.shape["pair"], ny, naux // ny),
        mesh=mesh,
        in_specs=level + level,
        out_specs=(amps, amps),
        check_vma=False,
    )
```

```python
import functools

import jax
import jax.numpy as jnp
from jax import lax
from jax.experimental import pallas as pl
from jax.experimental.pallas import tpu as pltpu
from jax.sharding import PartitionSpec as P

MESH = pl.DeviceIdType.MESH
F32, BF16, I32 = jnp.float32, jnp.bfloat16, jnp.int32
FIRST, DEPTH = 2, 3
VMEM = 36 * 1024 * 1024
CHUNKS = ((0, 5), (5, 10))


def halves(x):
    high = x.astype(BF16)
    return high, (x - high.astype(F32)).astype(BF16)


def dot(a, b, ca, cb):
    return lax.dot_general(a, b, (((ca,), (cb,)), ((), ())), preferred_element_type=F32)


def iota(shape, dim):
    return lax.broadcasted_iota(I32, shape, dim)


def cat(parts, axis):
    return jnp.concatenate(parts, axis=axis)


def hops(d, n):
    return min(d, n - d)


def kernel(
    npair, ny, nz,
    *refs,
):
    small_hbm, refs = refs[:12], refs[12:]
    small, refs = refs[8 : 8 + 12], refs[:8] + refs[8 + 12 :]
    body(npair, ny, nz, small_hbm, small, *refs)


def body(
    npair, ny, nz, small_hbm, small,
    la_hbm, ra_hbm, sa_hbm, le_hbm, re_hbm, se_hbm,
    out_a, out_e,
    la, ra, sa, le, re, se,
    gat, blk_a, blk_e, tot, cpl, bhl, wsel, wsel_e, amp_a, rec_a, amp_e, rec_e,
    send0, send1, recv0, recv1,
    small_sem, la_sem, ra_sem, le_sem, re_sem, sa_sem, se_sem,
    gat_s, gat_r, blk_s, blk_r, ble_s, ble_r, rs_s, rs_r,
):
    nbr_a, rank_a, fock_a, gap_a, nbr_e, rank_e, fock_e, gap_e = small[:8]
    amps_a, en_a, amps_e, en_e = small[8:]
    me, grp = lax.axis_index("aux"), lax.axis_index("pair")
    naux = ny * nz
    my, mz = me // nz, lax.rem(me, nz)
    count_a, rows_a, wide_a = amps_a.shape
    rows_e, count_e, wide_e = amps_e.shape
    nb = nbr_a.shape[0]
    lanes = wide_a
    start_a, start_e = me * rows_a, me * rows_e
    sends, recvs = (send0, send1), (recv0, recv1)

    far = sorted(
        ((dy, dz) for dy in range(ny) for dz in range(nz) if dy or dz),
        key=lambda o: -(hops(o[0], ny) + hops(o[1], nz)),
    )

    def peer_of(o):
        return lax.rem(my + o[0], ny) * nz + lax.rem(mz + o[1], nz)

    barrier = pltpu.get_barrier_semaphore()
    for o in far:
        pl.semaphore_signal(barrier, inc=1, device_id={"aux": peer_of(o)}, device_id_type=MESH)
    for d in range(1, npair):
        pl.semaphore_signal(
            barrier, inc=1, device_id={"pair": lax.rem(grp + d, npair)}, device_id_type=MESH
        )

    def load_pair(p):
        return (
            pltpu.make_async_copy(la_hbm.at[p], la.at[p], la_sem.at[p]),
            pltpu.make_async_copy(ra_hbm.at[p], ra.at[p], ra_sem.at[p]),
        )

    load_env = (
        pltpu.make_async_copy(le_hbm, le, le_sem),
        pltpu.make_async_copy(re_hbm, re, re_sem),
    )
    load_se = pltpu.make_async_copy(se_hbm, se, se_sem)
    load_sa = pltpu.make_async_copy(sa_hbm, sa, sa_sem)
    load_small = [
        pltpu.make_async_copy(src, dst, small_sem.at[i])
        for i, (src, dst) in enumerate(zip(small_hbm, small))
    ]
    for copy in load_small:
        copy.start()
    load_sa.start()
    load_se.start()
    for copy in load_env:
        copy.start()

    def start_pair(p):
        for copy in load_pair(p):
            copy.start()

    for p in range(FIRST):
        start_pair(p)
    for copy in load_small:
        copy.wait()

    row8, col8 = iota((rows_a, lanes), 0), iota((rows_a, lanes), 1)
    for p in range(count_a):
        inside = (start_a + row8 < rank_a[p]) & (col8 < rank_a[p])
        own = jnp.where(inside, amps_a[p].astype(F32), 0.0)
        amp_a[p] = own
        own = own.astype(BF16)
        gat[me, p] = own
        blk_a[grp * count_a + p] = own

    def own_env(q):
        rows = jnp.zeros((8, wide_e), F32)
        r, s = iota((8, wide_e), 0), iota((8, wide_e), 1)
        for i in range(rows_e):
            rows = jnp.where(r == i, amps_e[i, q : q + 1, :].astype(F32), rows)
        inside = (r < rows_e) & (start_e + r < rank_e[q]) & (s < rank_e[q])
        return jnp.where(inside, rows, 0.0), inside

    owns = [own_env(q) for q in range(count_e)]
    for q in range(count_e):
        at = grp * count_e + q
        blk_e[at] = jnp.zeros(blk_e.shape[1:], BF16)
        blk_e[at, :, :wide_e] = owns[q][0].astype(BF16)

    pl.semaphore_wait(barrier, naux + npair - 2)

    def to_aux(o):
        e = o[0] * nz + o[1]
        slot = gat.at[me]
        return pltpu.make_async_remote_copy(
            src_ref=slot, dst_ref=slot, send_sem=gat_s.at[e], recv_sem=gat_r.at[e],
            device_id={"aux": peer_of(o)}, device_id_type=MESH,
        )

    def to_pair(d, block, count, s, r):
        slot = block.at[pl.ds(grp * count, count)]
        return pltpu.make_async_remote_copy(
            src_ref=slot, dst_ref=slot, send_sem=s.at[d], recv_sem=r.at[d],
            device_id={"pair": lax.rem(grp + d, npair)}, device_id_type=MESH,
        )

    for d in range(1, npair):
        to_pair(d, blk_a, count_a, blk_s, blk_r).start()
        to_pair(d, blk_e, count_e, ble_s, ble_r).start()
    for o in far:
        to_aux(o).start()

    for p in range(FIRST, DEPTH):
        start_pair(p)

    for p in range(count_a):
        inside = (start_a + row8 < rank_a[p]) & (col8 < rank_a[p])
        across = jnp.broadcast_to(en_a[p : p + 1, :], (rows_a, lanes))
        down = jnp.sum(jnp.where(col8 == start_a + row8, across, 0.0), axis=1, keepdims=True)
        rec_a[p] = jnp.where(inside, 1.0 / (across + down + gap_a[p]), 0.0)
    r48, c48 = iota((8, wide_e), 0), iota((8, wide_e), 1)
    for q in range(count_e):
        across = jnp.broadcast_to(en_e[q : q + 1, :], (8, wide_e))
        down = jnp.sum(jnp.where(c48 == start_e + r48, across, 0.0), axis=1, keepdims=True)
        denom = jnp.where(r48 < rows_e, across + down + gap_e[q], 1.0)
        rec_e[q] = jnp.where(owns[q][1], 1.0 / denom, 0.0)
        amp_e[q] = owns[q][0]

    load_sa.wait()
    load_se.wait()
    group = nb * rows_a
    k_in, k_out = iota((nb * wide_a, lanes), 0), iota((nb * wide_a, lanes), 1)
    k_at = lax.rem(k_out, group)
    source = (k_at // rows_a) * wide_a + start_a + lax.rem(k_at, rows_a)
    pick = jnp.where((k_in == source) & (k_out < 2 * group), 1.0, 0.0).astype(BF16)

    def overs(p):
        return cat([sa[p, k] for k in range(nb)], 1)

    for p in range(count_a):
        wsel[p] = dot(overs(p), pick, 1, 0).astype(BF16)

    pin, pout = iota((wide_e, lanes), 0), iota((wide_e, lanes), 1)
    pat = lax.rem(pout, 64)
    inner = lax.rem(pat, 8)
    for h in range(count_e // 2):
        chosen = jnp.zeros((wide_e, lanes), F32)
        for k in range(nb):
            for b in range(2):
                sel = jnp.where(
                    (pin == start_e + inner) & (inner < rows_e) & (pat // 8 == 2 * k + b), 1.0, 0.0
                ).astype(BF16)
                chosen = chosen + dot(se[2 * h + b, k], sel, 1, 0)
        wsel_e[h] = chosen.astype(BF16)

    for copy in load_env:
        copy.wait()
    le_all = le[...].reshape(count_e * wide_e, le.shape[2])
    pad = 64 - wide_e
    gap_rows = jnp.zeros((pad, re.shape[2]), BF16)
    re_all = cat([x for q in range(count_e) for x in (re[q], gap_rows)], 0)
    base_e = dot(le_all, re_all, 1, 1)
    low_lanes = iota((wide_e, lanes), 1) < 64
    base_h = []
    for h in range(count_e // 2):
        block = base_e[:, h * lanes : (h + 1) * lanes]
        a, b = 2 * h * wide_e, (2 * h + 1) * wide_e
        base_h.append(jnp.where(low_lanes, block[a : a + wide_e], block[b : b + wide_e]))

    def ladder(p):
        if not isinstance(p, int):
            start_pair(p + DEPTH)
        for copy in load_pair(p):
            copy.wait()
        base = dot(la[p], ra[p], 1, 1)
        tot[p] = base
        bhl[p] = cat(halves(base), 0)

    pl.loop(0, count_a - DEPTH)(ladder)
    for p in range(count_a - DEPTH, count_a - 3):
        ladder(p)

    lane_k = iota((wide_a, 2 * group), 1)
    at_k = lax.rem(lane_k, group) // rows_a
    zero = jnp.zeros((rows_a, wide_a), F32)

    def couple(p):
        rows, scale = [], jnp.zeros((wide_a, 2 * group), F32)
        for k in range(nb):
            near = blk_a[nbr_a[k, p]].astype(F32)
            rows.append(cat([near if i == k else zero for i in range(nb)], 1))
            scale = jnp.where(at_k == k, fock_a[k, p], scale)
        rows = cat(rows, 0).astype(BF16)
        right = dot(overs(p), cat([rows, rows], 0), 1, 1) * scale
        high = right.astype(BF16).astype(F32)
        right = jnp.where(lane_k < group, high, right - high).astype(BF16)
        cpl[p] = dot(wsel[p][:, : 2 * group], right, 1, 1)

    fill = jnp.zeros((pad, wide_e), BF16)
    lane16, row16 = iota((16, lanes), 1), iota((16, lanes), 0)
    keep16 = (lane16 < 64) == (row16 < 8)

    def couple_env(h):
        q0, q1 = 2 * h, 2 * h + 1
        parts = []
        for k in range(nb):
            both = cat([se[q0, k], fill, se[q1, k], fill], 0)
            rows = cat(
                [blk_e[nbr_e[q, k], :, :wide_e].astype(F32) for q in (q0, q1)], 0
            ).astype(BF16)
            prod = dot(rows, both, 1, 1)
            scale = jnp.where(row16 < 8, fock_e[q0, k], fock_e[q1, k])
            parts.append(jnp.where(keep16, prod * scale, 0.0))
        near = cat(halves(cat(parts, 0)), 0)
        return (base_h[h] + dot(wsel_e[h], near, 1, 0)).astype(BF16)

    @pl.loop(1, npair)
    def _(d):
        to_pair(d, blk_a, count_a, blk_s, blk_r).wait()
        to_pair(d, blk_e, count_e, ble_s, ble_r).wait()

    for p in range(count_a // 2):
        couple(p)
    ladder(7)
    both_e = cat([couple_env(h) for h in range(count_e // 2)], 0)
    srow, scol = iota((lanes, 2 * wide_e), 0), iota((lanes, 2 * wide_e), 1)
    sj, sr = srow // 8, lax.rem(srow, 8)
    si = lax.rem(sr, 4)
    spread = jnp.where(
        (scol == (sr // 4) * wide_e + rows_e * sj + si) & (si < rows_e), 1.0, 0.0
    ).astype(BF16)
    packed = dot(spread, both_e, 1, 0)
    for j in range(naux):
        send1[j, CHUNKS[1][1] - CHUNKS[1][0]] = packed[8 * j : 8 * j + 8].astype(BF16)
    ladder(8)
    for p in range(count_a // 2, count_a):
        couple(p)
    ladder(9)

    def sums_to(c, o):
        e = o[0] * nz + o[1]
        return pltpu.make_async_remote_copy(
            src_ref=sends[c].at[peer_of(o)], dst_ref=recvs[c].at[e],
            send_sem=rs_s.at[c, e], recv_sem=rs_r.at[c, e],
            device_id={"aux": peer_of(o)}, device_id_type=MESH,
        )

    for c, (lo, hi) in enumerate(CHUNKS):
        if c == 0:
            for o in far:
                to_aux(o).wait()
        for p in range(lo, hi):
            amp = gat[:, p].astype(F32).reshape(wide_a, wide_a).astype(BF16)
            x = dot(cat([amp, amp], 0), bhl[p], 0, 0)
            y = dot(cat(halves(x), 1), cat([amp, amp], 1), 1, 1)
            total = (tot[p] + cpl[p] + x + y).reshape(naux, rows_a, wide_a)
            sends[c][:, p - lo] = total.astype(BF16)
        for o in far:
            sums_to(c, o).start()

    near_first = far[::-1]
    for c, (lo, hi) in enumerate(CHUNKS):
        acc = sends[c][me].astype(F32)
        for o in near_first:
            sums_to(c, o).wait()
            acc = acc + recvs[c][o[0] * nz + o[1]].astype(F32)
        for p in range(lo, hi):
            out_a[p] = amp_a[p] - acc[p - lo] * rec_a[p]
        if c == 1:
            env = acc[hi - lo]
            turned = pltpu.roll(env, 64, 1)
            for q in range(count_e):
                r = 4 * (q // 2)
                block = (env if q % 2 == 0 else turned)[r : r + 4, :wide_e]
                new = amp_e[q][:4] - block * rec_e[q][:4]
                for i in range(rows_e):
                    out_e[i, q : q + 1, :] = new[i : i + 1]


def shards(
    npair, ny, nz,
    left_active, right_active, amps_active, rank_active, gap_active, energy_active,
    intersect_active, fock_active, neighbor_active,
    left_env, right_env, amps_env, rank_env, gap_env, energy_env,
    intersect_env, fock_env, neighbor_env,
):
    naux = ny * nz
    count_a, rows_a, wide_a = amps_active.shape
    count_e, rows_e, wide_e = amps_env.shape
    nb = neighbor_active.shape[1]
    vmem = pl.BlockSpec(memory_space=pltpu.VMEM)
    hbm = pl.BlockSpec(memory_space=pltpu.HBM)
    dma = pltpu.SemaphoreType.DMA
    n0 = CHUNKS[0][1] - CHUNKS[0][0]
    n1 = CHUNKS[1][1] - CHUNKS[1][0]
    small = (
        neighbor_active.T, rank_active, fock_active.T, gap_active,
        neighbor_env, rank_env, fock_env, gap_env,
        amps_active, energy_active, amps_env.transpose(1, 0, 2), energy_env,
    )
    new_active, new_env = pl.pallas_call(
        functools.partial(kernel, npair, ny, nz),
        out_shape=(
            jax.ShapeDtypeStruct((count_a, rows_a, wide_a), F32),
            jax.ShapeDtypeStruct((rows_e, count_e, wide_e), F32),
        ),
        in_specs=[hbm] * 18,
        out_specs=(vmem, vmem),
        scratch_shapes=[pltpu.SMEM(x.shape, x.dtype) for x in small[:8]]
        + [pltpu.VMEM(x.shape, x.dtype) for x in small[8:]]
        + [
            pltpu.VMEM(left_active.shape, BF16),
            pltpu.VMEM(right_active.shape, BF16),
            pltpu.VMEM(intersect_active.shape, BF16),
            pltpu.VMEM(left_env.shape, BF16),
            pltpu.VMEM(right_env.shape, BF16),
            pltpu.VMEM(intersect_env.shape, BF16),
            pltpu.VMEM((naux, count_a, rows_a, wide_a), BF16),
            pltpu.VMEM((npair * count_a, rows_a, wide_a), BF16),
            pltpu.VMEM((npair * count_e, 8, 128), BF16),
            pltpu.VMEM((count_a, wide_a, wide_a), F32),
            pltpu.VMEM((count_a, wide_a, wide_a), F32),
            pltpu.VMEM((count_a, 2 * wide_a, wide_a), BF16),
            pltpu.VMEM((count_a, wide_a, 128), BF16),
            pltpu.VMEM((count_e // 2, wide_e, 128), BF16),
            pltpu.VMEM((count_a, rows_a, wide_a), F32),
            pltpu.VMEM((count_a, rows_a, wide_a), F32),
            pltpu.VMEM((count_e, 8, wide_e), F32),
            pltpu.VMEM((count_e, 8, wide_e), F32),
            pltpu.VMEM((naux, n0, rows_a, wide_a), BF16),
            pltpu.VMEM((naux, n1 + 1, rows_a, wide_a), BF16),
            pltpu.VMEM((naux, n0, rows_a, wide_a), BF16),
            pltpu.VMEM((naux, n1 + 1, rows_a, wide_a), BF16),
            dma((12,)), dma((count_a,)), dma((count_a,)), dma, dma, dma, dma,
            dma((naux,)), dma((naux,)),
            dma((npair,)), dma((npair,)), dma((npair,)), dma((npair,)),
            dma((2, naux)), dma((2, naux)),
        ],
        compiler_params=pltpu.CompilerParams(
            collective_id=0, has_side_effects=True, vmem_limit_bytes=VMEM
        ),
    )(
        *(
            pltpu.with_memory_space_constraint(x, pltpu.HBM)
            for x in small
            + (left_active, right_active, intersect_active, left_env, right_env, intersect_env)
        )
    )
    return new_active, new_env.transpose(1, 0, 2)


def solution(mesh):
    ints, amps = P("pair", None, "aux"), P("pair", "aux", None)
    one, two, four = P("pair"), P("pair", None), P("pair", None, None, None)
    level = (ints, ints, amps, one, one, two, four, two, two)
    naux = mesh.shape["aux"]
    ny = next(n for n in range(int(naux**0.5), 0, -1) if naux % n == 0)
    return jax.shard_map(
        functools.partial(shards, mesh.shape["pair"], ny, naux // ny),
        mesh=mesh,
        in_specs=level + level,
        out_specs=(amps, amps),
        check_vma=False,
    )
```

```python
import functools

import jax
import jax.numpy as jnp
from jax import lax
from jax.experimental import pallas as pl
from jax.experimental.pallas import tpu as pltpu
from jax.sharding import PartitionSpec as P

MESH = pl.DeviceIdType.MESH
F32, BF16, I32 = jnp.float32, jnp.bfloat16, jnp.int32
FIRST, DEPTH = 2, 5
VMEM = 36 * 1024 * 1024
CHUNKS = ((0, 5), (5, 10))


def halves(x):
    high = x.astype(BF16)
    return high, (x - high.astype(F32)).astype(BF16)


def dot(a, b, ca, cb):
    return lax.dot_general(a, b, (((ca,), (cb,)), ((), ())), preferred_element_type=F32)


def iota(shape, dim):
    return lax.broadcasted_iota(I32, shape, dim)


def cat(parts, axis):
    return jnp.concatenate(parts, axis=axis)


def hops(d, n):
    return min(d, n - d)


def kernel(
    npair, ny, nz,
    *refs,
):
    small_hbm, refs = refs[:12], refs[12:]
    small, refs = refs[8 : 8 + 12], refs[:8] + refs[8 + 12 :]
    body(npair, ny, nz, small_hbm, small, *refs)


def body(
    npair, ny, nz, small_hbm, small,
    la_hbm, ra_hbm, sa_hbm, le_hbm, re_hbm, se_hbm,
    out_a, out_e,
    la, ra, sa, le, re, se,
    gat, blk_a, blk_e, tot, b16, near, wsel, wsel_e, amp_a, rec_a, amp_e, rec_e,
    send0, send1, recv0, recv1,
    small_sem, la_sem, ra_sem, le_sem, re_sem, sa_sem, se_sem,
    gat_s, gat_r, blk_s, blk_r, ble_s, ble_r, rs_s, rs_r,
):
    nbr_a, rank_a, fock_a, gap_a, nbr_e, rank_e, fock_e, gap_e = small[:8]
    amps_a, en_a, amps_e, en_e = small[8:]
    me, grp = lax.axis_index("aux"), lax.axis_index("pair")
    naux = ny * nz
    my, mz = me // nz, lax.rem(me, nz)
    count_a, rows_a, wide_a = amps_a.shape
    rows_e, count_e, wide_e = amps_e.shape
    nb = nbr_a.shape[0]
    lanes = wide_a
    start_a, start_e = me * rows_a, me * rows_e
    sends, recvs = (send0, send1), (recv0, recv1)

    far = sorted(
        ((dy, dz) for dy in range(ny) for dz in range(nz) if dy or dz),
        key=lambda o: -(hops(o[0], ny) + hops(o[1], nz)),
    )

    def peer_of(o):
        return lax.rem(my + o[0], ny) * nz + lax.rem(mz + o[1], nz)

    barrier = pltpu.get_barrier_semaphore()
    for o in far:
        pl.semaphore_signal(barrier, inc=1, device_id={"aux": peer_of(o)}, device_id_type=MESH)
    for d in range(1, npair):
        pl.semaphore_signal(
            barrier, inc=1, device_id={"pair": lax.rem(grp + d, npair)}, device_id_type=MESH
        )

    def load_pair(p):
        return (
            pltpu.make_async_copy(la_hbm.at[p], la.at[p], la_sem.at[p]),
            pltpu.make_async_copy(ra_hbm.at[p], ra.at[p], ra_sem.at[p]),
        )

    load_env = (
        pltpu.make_async_copy(le_hbm, le, le_sem),
        pltpu.make_async_copy(re_hbm, re, re_sem),
    )
    load_se = pltpu.make_async_copy(se_hbm, se, se_sem)
    load_sa = pltpu.make_async_copy(sa_hbm, sa, sa_sem)
    load_small = [
        pltpu.make_async_copy(src, dst, small_sem.at[i])
        for i, (src, dst) in enumerate(zip(small_hbm, small))
    ]
    for copy in load_small:
        copy.start()
    load_sa.start()
    load_se.start()
    for copy in load_env:
        copy.start()

    def start_pair(p):
        for copy in load_pair(p):
            copy.start()

    for p in range(FIRST):
        start_pair(p)
    for copy in load_small:
        copy.wait()

    row8, col8 = iota((rows_a, lanes), 0), iota((rows_a, lanes), 1)
    for p in range(count_a):
        inside = (start_a + row8 < rank_a[p]) & (col8 < rank_a[p])
        own = jnp.where(inside, amps_a[p].astype(F32), 0.0)
        amp_a[p] = own
        own = own.astype(BF16)
        gat[me, p] = own
        blk_a[grp * count_a + p] = own

    def own_env(q):
        rows = jnp.zeros((8, wide_e), F32)
        r, s = iota((8, wide_e), 0), iota((8, wide_e), 1)
        for i in range(rows_e):
            rows = jnp.where(r == i, amps_e[i, q : q + 1, :].astype(F32), rows)
        inside = (r < rows_e) & (start_e + r < rank_e[q]) & (s < rank_e[q])
        return jnp.where(inside, rows, 0.0), inside

    owns = [own_env(q) for q in range(count_e)]
    for q in range(count_e):
        at = grp * count_e + q
        blk_e[at] = jnp.zeros(blk_e.shape[1:], BF16)
        blk_e[at, :, :wide_e] = owns[q][0].astype(BF16)

    pl.semaphore_wait(barrier, naux + npair - 2)

    def to_aux(o):
        slot = gat.at[me]
        return pltpu.make_async_remote_copy(
            src_ref=slot, dst_ref=slot, send_sem=gat_s, recv_sem=gat_r,
            device_id={"aux": peer_of(o)}, device_id_type=MESH,
        )

    def arrived(ref, send, recv):
        pltpu.make_async_remote_copy(
            src_ref=ref, dst_ref=ref, send_sem=send, recv_sem=recv,
            device_id={"aux": peer_of(far[0])}, device_id_type=MESH,
        ).wait()

    def to_pair(d, block, count, s, r):
        slot = block.at[pl.ds(grp * count, count)]
        return pltpu.make_async_remote_copy(
            src_ref=slot, dst_ref=slot, send_sem=s, recv_sem=r,
            device_id={"pair": lax.rem(grp + d, npair)}, device_id_type=MESH,
        )

    for d in range(1, npair):
        to_pair(d, blk_a, count_a, blk_s, blk_r).start()
        to_pair(d, blk_e, count_e, ble_s, ble_r).start()
    for o in far:
        to_aux(o).start()

    for p in range(FIRST, DEPTH):
        start_pair(p)

    for p in range(count_a):
        inside = (start_a + row8 < rank_a[p]) & (col8 < rank_a[p])
        across = jnp.broadcast_to(en_a[p : p + 1, :], (rows_a, lanes))
        down = jnp.sum(jnp.where(col8 == start_a + row8, across, 0.0), axis=1, keepdims=True)
        rec_a[p] = jnp.where(inside, 1.0 / (across + down + gap_a[p]), 0.0)
    r48, c48 = iota((8, wide_e), 0), iota((8, wide_e), 1)
    for q in range(count_e):
        across = jnp.broadcast_to(en_e[q : q + 1, :], (8, wide_e))
        down = jnp.sum(jnp.where(c48 == start_e + r48, across, 0.0), axis=1, keepdims=True)
        denom = jnp.where(r48 < rows_e, across + down + gap_e[q], 1.0)
        rec_e[q] = jnp.where(owns[q][1], 1.0 / denom, 0.0)
        amp_e[q] = owns[q][0]

    load_sa.wait()
    load_se.wait()
    group = nb * rows_a
    k_in, k_out = iota((nb * wide_a, lanes), 0), iota((nb * wide_a, lanes), 1)
    k_at = lax.rem(k_out, group)
    source = (k_at // rows_a) * wide_a + start_a + lax.rem(k_at, rows_a)
    pick = jnp.where((k_in == source) & (k_out < group), 1.0, 0.0).astype(BF16)

    def overs(p):
        return cat([sa[p, k] for k in range(nb)], 1)

    for p in range(count_a):
        wsel[p] = dot(overs(p), pick, 1, 0).astype(BF16)

    pin, pout = iota((wide_e, lanes), 0), iota((wide_e, lanes), 1)
    pat = lax.rem(pout, 64)
    inner = lax.rem(pat, 8)
    for h in range(count_e // 2):
        chosen = jnp.zeros((wide_e, lanes), F32)
        for k in range(nb):
            for b in range(2):
                sel = jnp.where(
                    (pin == start_e + inner) & (inner < rows_e) & (pat // 8 == 2 * k + b), 1.0, 0.0
                ).astype(BF16)
                chosen = chosen + dot(se[2 * h + b, k], sel, 1, 0)
        wsel_e[h] = chosen.astype(BF16)

    for copy in load_env:
        copy.wait()
    le_all = le[...].reshape(count_e * wide_e, le.shape[2])
    pad = 64 - wide_e
    gap_rows = jnp.zeros((pad, re.shape[2]), BF16)
    re_all = cat([x for q in range(count_e) for x in (re[q], gap_rows)], 0)
    base_e = dot(le_all, re_all, 1, 1)
    low_lanes = iota((wide_e, lanes), 1) < 64
    base_h = []
    for h in range(count_e // 2):
        block = base_e[:, h * lanes : (h + 1) * lanes]
        a, b = 2 * h * wide_e, (2 * h + 1) * wide_e
        base_h.append(jnp.where(low_lanes, block[a : a + wide_e], block[b : b + wide_e]))

    def ladder(p):
        if not isinstance(p, int):
            start_pair(p + DEPTH)
        for copy in load_pair(p):
            copy.wait()
        base = dot(la[p], ra[p], 1, 1)
        tot[p] = base
        b16[p] = base.astype(BF16)

    pl.loop(0, count_a - DEPTH)(ladder)
    for p in range(count_a - DEPTH, count_a - 3):
        ladder(p)

    at_k = iota((1, lanes), 1) // rows_a
    zero = jnp.zeros((rows_a, wide_a), F32)
    rest = jnp.zeros((lanes - group, nb * wide_a), BF16)

    def couple(p):
        rows, scale = [], jnp.zeros((1, lanes), F32)
        for k in range(nb):
            nbr = blk_a[nbr_a[k, p]].astype(F32)
            rows.append(cat([nbr if i == k else zero for i in range(nb)], 1))
            scale = jnp.where(at_k == k, fock_a[k, p], scale)
        rows = cat([cat(rows, 0).astype(BF16), rest], 0)
        near[p] = (dot(overs(p), rows, 1, 1) * scale).astype(BF16)

    fill = jnp.zeros((pad, wide_e), BF16)
    lane16, row16 = iota((16, lanes), 1), iota((16, lanes), 0)
    keep16 = (lane16 < 64) == (row16 < 8)

    def couple_env(h):
        q0, q1 = 2 * h, 2 * h + 1
        parts = []
        for k in range(nb):
            both = cat([se[q0, k], fill, se[q1, k], fill], 0)
            rows = cat(
                [blk_e[nbr_e[q, k], :, :wide_e].astype(F32) for q in (q0, q1)], 0
            ).astype(BF16)
            prod = dot(rows, both, 1, 1)
            scale = jnp.where(row16 < 8, fock_e[q0, k], fock_e[q1, k])
            parts.append(jnp.where(keep16, prod * scale, 0.0))
        near = cat(halves(cat(parts, 0)), 0)
        return (base_h[h] + dot(wsel_e[h], near, 1, 0)).astype(BF16)

    arrived(blk_a.at[pl.ds(0, (npair - 1) * count_a)], blk_s, blk_r)
    arrived(blk_e.at[pl.ds(0, (npair - 1) * count_e)], ble_s, ble_r)

    for p in range(count_a):
        couple(p)
    def sums_to(c, o):
        e = o[0] * nz + o[1]
        return pltpu.make_async_remote_copy(
            src_ref=sends[c].at[peer_of(o)], dst_ref=recvs[c].at[e],
            send_sem=rs_s.at[c], recv_sem=rs_r.at[c],
            device_id={"aux": peer_of(o)}, device_id_type=MESH,
        )

    for c, (lo, hi) in enumerate(CHUNKS):
        if c == 0:
            arrived(gat.at[pl.ds(0, naux - 1)], gat_s, gat_r)
        for p in range(lo, hi):
            amp = gat[:, p].astype(F32).reshape(wide_a, wide_a).astype(BF16)
            x = dot(amp, b16[p], 0, 0)
            y = dot(cat([x.astype(BF16), wsel[p]], 1), cat([amp, near[p]], 1), 1, 1)
            total = (tot[p] + x + y).reshape(naux, rows_a, wide_a)
            sends[c][:, p - lo] = total.astype(BF16)
        for o in far:
            sums_to(c, o).start()
        if c == 0:
            both_e = cat([couple_env(h) for h in range(count_e // 2)], 0)
            srow, scol = iota((lanes, 2 * wide_e), 0), iota((lanes, 2 * wide_e), 1)
            sj, sr = srow // 8, lax.rem(srow, 8)
            si = lax.rem(sr, 4)
            spread = jnp.where(
                (scol == (sr // 4) * wide_e + rows_e * sj + si) & (si < rows_e), 1.0, 0.0
            ).astype(BF16)
            packed = dot(spread, both_e, 1, 0)
            for j in range(naux):
                send1[j, CHUNKS[1][1] - CHUNKS[1][0]] = packed[8 * j : 8 * j + 8].astype(BF16)
            for p in range(count_a - 3, count_a):
                for copy in load_pair(p):
                    copy.wait()
            for p in range(count_a - 3, count_a):
                base = dot(la[p], ra[p], 1, 1)
                tot[p] = base
                b16[p] = base.astype(BF16)

    for c, (lo, hi) in enumerate(CHUNKS):
        arrived(recvs[c].at[pl.ds(1, naux - 1)], rs_s.at[c], rs_r.at[c])
        acc = sends[c][me].astype(F32)
        for e in range(1, naux):
            acc = acc + recvs[c][e].astype(F32)
        for p in range(lo, hi):
            out_a[p] = amp_a[p] - acc[p - lo] * rec_a[p]
        if c == 1:
            env = acc[hi - lo]
            turned = pltpu.roll(env, 64, 1)
            for q in range(count_e):
                r = 4 * (q // 2)
                block = (env if q % 2 == 0 else turned)[r : r + 4, :wide_e]
                new = amp_e[q][:4] - block * rec_e[q][:4]
                for i in range(rows_e):
                    out_e[i, q : q + 1, :] = new[i : i + 1]


def shards(
    npair, ny, nz,
    left_active, right_active, amps_active, rank_active, gap_active, energy_active,
    intersect_active, fock_active, neighbor_active,
    left_env, right_env, amps_env, rank_env, gap_env, energy_env,
    intersect_env, fock_env, neighbor_env,
):
    naux = ny * nz
    count_a, rows_a, wide_a = amps_active.shape
    count_e, rows_e, wide_e = amps_env.shape
    nb = neighbor_active.shape[1]
    vmem = pl.BlockSpec(memory_space=pltpu.VMEM)
    hbm = pl.BlockSpec(memory_space=pltpu.HBM)
    dma = pltpu.SemaphoreType.DMA
    n0 = CHUNKS[0][1] - CHUNKS[0][0]
    n1 = CHUNKS[1][1] - CHUNKS[1][0]
    small = (
        neighbor_active.T, rank_active, fock_active.T, gap_active,
        neighbor_env, rank_env, fock_env, gap_env,
        amps_active, energy_active, amps_env.transpose(1, 0, 2), energy_env,
    )
    new_active, new_env = pl.pallas_call(
        functools.partial(kernel, npair, ny, nz),
        out_shape=(
            jax.ShapeDtypeStruct((count_a, rows_a, wide_a), F32),
            jax.ShapeDtypeStruct((rows_e, count_e, wide_e), F32),
        ),
        in_specs=[hbm] * 18,
        out_specs=(vmem, vmem),
        scratch_shapes=[pltpu.SMEM(x.shape, x.dtype) for x in small[:8]]
        + [pltpu.VMEM(x.shape, x.dtype) for x in small[8:]]
        + [
            pltpu.VMEM(left_active.shape, BF16),
            pltpu.VMEM(right_active.shape, BF16),
            pltpu.VMEM(intersect_active.shape, BF16),
            pltpu.VMEM(left_env.shape, BF16),
            pltpu.VMEM(right_env.shape, BF16),
            pltpu.VMEM(intersect_env.shape, BF16),
            pltpu.VMEM((naux, count_a, rows_a, wide_a), BF16),
            pltpu.VMEM((npair * count_a, rows_a, wide_a), BF16),
            pltpu.VMEM((npair * count_e, 8, 128), BF16),
            pltpu.VMEM((count_a, wide_a, wide_a), F32),
            pltpu.VMEM((count_a, wide_a, wide_a), BF16),
            pltpu.VMEM((count_a, wide_a, wide_a), BF16),
            pltpu.VMEM((count_a, wide_a, 128), BF16),
            pltpu.VMEM((count_e // 2, wide_e, 128), BF16),
            pltpu.VMEM((count_a, rows_a, wide_a), F32),
            pltpu.VMEM((count_a, rows_a, wide_a), F32),
            pltpu.VMEM((count_e, 8, wide_e), F32),
            pltpu.VMEM((count_e, 8, wide_e), F32),
            pltpu.VMEM((naux, n0, rows_a, wide_a), BF16),
            pltpu.VMEM((naux, n1 + 1, rows_a, wide_a), BF16),
            pltpu.VMEM((naux, n0, rows_a, wide_a), BF16),
            pltpu.VMEM((naux, n1 + 1, rows_a, wide_a), BF16),
            dma((12,)), dma((count_a,)), dma((count_a,)), dma, dma, dma, dma,
            dma, dma, dma, dma, dma, dma, dma((2,)), dma((2,)),
        ],
        compiler_params=pltpu.CompilerParams(
            collective_id=0, has_side_effects=True, vmem_limit_bytes=VMEM
        ),
    )(
        *(
            pltpu.with_memory_space_constraint(x, pltpu.HBM)
            for x in small
            + (left_active, right_active, intersect_active, left_env, right_env, intersect_env)
        )
    )
    return new_active, new_env.transpose(1, 0, 2)


def solution(mesh):
    ints, amps = P("pair", None, "aux"), P("pair", "aux", None)
    one, two, four = P("pair"), P("pair", None), P("pair", None, None, None)
    level = (ints, ints, amps, one, one, two, four, two, two)
    naux = mesh.shape["aux"]
    ny = next(n for n in range(int(naux**0.5), 0, -1) if naux % n == 0)
    return jax.shard_map(
        functools.partial(shards, mesh.shape["pair"], ny, naux // ny),
        mesh=mesh,
        in_specs=level + level,
        out_specs=(amps, amps),
        check_vma=False,
    )
```

```python
import functools

import jax
import jax.numpy as jnp
from jax import lax
from jax.experimental import pallas as pl
from jax.experimental.pallas import tpu as pltpu
from jax.sharding import PartitionSpec as P

MESH = pl.DeviceIdType.MESH
F32, BF16, I32 = jnp.float32, jnp.bfloat16, jnp.int32
FIRST, DEPTH = 2, 5
VMEM = 36 * 1024 * 1024
CHUNKS = ((0, 6), (6, 10))


def halves(x):
    high = x.astype(BF16)
    return high, (x - high.astype(F32)).astype(BF16)


def dot(a, b, ca, cb):
    return lax.dot_general(a, b, (((ca,), (cb,)), ((), ())), preferred_element_type=F32)


def iota(shape, dim):
    return lax.broadcasted_iota(I32, shape, dim)


def cat(parts, axis):
    return jnp.concatenate(parts, axis=axis)


def hops(d, n):
    return min(d, n - d)


def kernel(
    npair, ny, nz,
    *refs,
):
    small_hbm, refs = refs[:12], refs[12:]
    small, refs = refs[8 : 8 + 12], refs[:8] + refs[8 + 12 :]
    body(npair, ny, nz, small_hbm, small, *refs)


def body(
    npair, ny, nz, small_hbm, small,
    la_hbm, ra_hbm, sa_hbm, le_hbm, re_hbm, se_hbm,
    out_a, out_e,
    la, ra, sa, le, re, se,
    gat0, gat1, blk_a, blk_e, tot, b16, near, ampb, turn, wsel, wsel_e, amp_a, rec_a, amp_e, rec_e,
    send0, send1, recv0, recv1,
    small_sem, la_sem, ra_sem, le_sem, re_sem, sa_sem, se_sem,
    gat_s, gat_r, blk_s, blk_r, ble_s, ble_r, rs_s, rs_r,
):
    nbr_a, rank_a, fock_a, gap_a, nbr_e, rank_e, fock_e, gap_e = small[:8]
    amps_a, en_a, amps_e, en_e = small[8:]
    me, grp = lax.axis_index("aux"), lax.axis_index("pair")
    naux = ny * nz
    my, mz = me // nz, lax.rem(me, nz)
    count_a, rows_a, wide_a = amps_a.shape
    rows_e, count_e, wide_e = amps_e.shape
    nb = nbr_a.shape[0]
    lanes = wide_a
    start_a, start_e = me * rows_a, me * rows_e
    gats = (gat0, gat1)
    sends, recvs = (send0, send1), (recv0, recv1)

    far = sorted(
        ((dy, dz) for dy in range(ny) for dz in range(nz) if dy or dz),
        key=lambda o: -(hops(o[0], ny) + hops(o[1], nz)),
    )

    def peer_of(o):
        return lax.rem(my + o[0], ny) * nz + lax.rem(mz + o[1], nz)

    barrier = pltpu.get_barrier_semaphore()
    for o in far:
        pl.semaphore_signal(barrier, inc=1, device_id={"aux": peer_of(o)}, device_id_type=MESH)
    for d in range(1, npair):
        pl.semaphore_signal(
            barrier, inc=1, device_id={"pair": lax.rem(grp + d, npair)}, device_id_type=MESH
        )

    def load_pair(p):
        return (
            pltpu.make_async_copy(la_hbm.at[p], la.at[p], la_sem.at[p]),
            pltpu.make_async_copy(ra_hbm.at[p], ra.at[p], ra_sem.at[p]),
        )

    load_env = (
        pltpu.make_async_copy(le_hbm, le, le_sem),
        pltpu.make_async_copy(re_hbm, re, re_sem),
    )
    load_se = pltpu.make_async_copy(se_hbm, se, se_sem)
    load_sa = pltpu.make_async_copy(sa_hbm, sa, sa_sem)
    load_small = [
        pltpu.make_async_copy(src, dst, small_sem.at[i])
        for i, (src, dst) in enumerate(zip(small_hbm, small))
    ]
    for copy in load_small:
        copy.start()
    load_sa.start()
    load_se.start()
    for copy in load_env:
        copy.start()

    def start_pair(p):
        for copy in load_pair(p):
            copy.start()

    for p in range(FIRST):
        start_pair(p)
    for copy in load_small:
        copy.wait()

    row8, col8 = iota((rows_a, lanes), 0), iota((rows_a, lanes), 1)
    for p in range(count_a):
        inside = (start_a + row8 < rank_a[p]) & (col8 < rank_a[p])
        own = jnp.where(inside, amps_a[p].astype(F32), 0.0)
        amp_a[p] = own
        own = own.astype(BF16)
        c = 0 if p < CHUNKS[0][1] else 1
        gats[c][me, p - CHUNKS[c][0]] = own
        blk_a[grp * count_a + p] = own

    def own_env(q):
        rows = jnp.zeros((8, wide_e), F32)
        r, s = iota((8, wide_e), 0), iota((8, wide_e), 1)
        for i in range(rows_e):
            rows = jnp.where(r == i, amps_e[i, q : q + 1, :].astype(F32), rows)
        inside = (r < rows_e) & (start_e + r < rank_e[q]) & (s < rank_e[q])
        return jnp.where(inside, rows, 0.0), inside

    owns = [own_env(q) for q in range(count_e)]
    for q in range(count_e):
        at = grp * count_e + q
        blk_e[at] = jnp.zeros(blk_e.shape[1:], BF16)
        blk_e[at, :, :wide_e] = owns[q][0].astype(BF16)

    pl.semaphore_wait(barrier, naux + npair - 2)

    def to_aux(c, o):
        slot = gats[c].at[me]
        return pltpu.make_async_remote_copy(
            src_ref=slot, dst_ref=slot, send_sem=gat_s.at[c], recv_sem=gat_r.at[c],
            device_id={"aux": peer_of(o)}, device_id_type=MESH,
        )

    def arrived(ref, send, recv):
        pltpu.make_async_remote_copy(
            src_ref=ref, dst_ref=ref, send_sem=send, recv_sem=recv,
            device_id={"aux": peer_of(far[0])}, device_id_type=MESH,
        ).wait()

    def to_pair(d, block, count, s, r):
        slot = block.at[pl.ds(grp * count, count)]
        return pltpu.make_async_remote_copy(
            src_ref=slot, dst_ref=slot, send_sem=s, recv_sem=r,
            device_id={"pair": lax.rem(grp + d, npair)}, device_id_type=MESH,
        )

    for d in range(1, npair):
        to_pair(d, blk_a, count_a, blk_s, blk_r).start()
        to_pair(d, blk_e, count_e, ble_s, ble_r).start()
    for c in range(2):
        for o in far:
            to_aux(c, o).start()

    for p in range(FIRST, DEPTH):
        start_pair(p)

    for p in range(count_a):
        inside = (start_a + row8 < rank_a[p]) & (col8 < rank_a[p])
        across = jnp.broadcast_to(en_a[p : p + 1, :], (rows_a, lanes))
        down = jnp.sum(jnp.where(col8 == start_a + row8, across, 0.0), axis=1, keepdims=True)
        rec_a[p] = jnp.where(inside, 1.0 / (across + down + gap_a[p]), 0.0)
    r48, c48 = iota((8, wide_e), 0), iota((8, wide_e), 1)
    for q in range(count_e):
        across = jnp.broadcast_to(en_e[q : q + 1, :], (8, wide_e))
        down = jnp.sum(jnp.where(c48 == start_e + r48, across, 0.0), axis=1, keepdims=True)
        denom = jnp.where(r48 < rows_e, across + down + gap_e[q], 1.0)
        rec_e[q] = jnp.where(owns[q][1], 1.0 / denom, 0.0)
        amp_e[q] = owns[q][0]

    load_sa.wait()
    load_se.wait()
    group = nb * rows_a
    k_in, k_out = iota((nb * wide_a, lanes), 0), iota((nb * wide_a, lanes), 1)
    k_at = lax.rem(k_out, group)
    source = (k_at // rows_a) * wide_a + start_a + lax.rem(k_at, rows_a)
    pick = jnp.where((k_in == source) & (k_out < group), 1.0, 0.0).astype(BF16)

    def overs(p):
        return cat([sa[p, k] for k in range(nb)], 1)

    for p in range(count_a):
        wsel[p] = dot(overs(p), pick, 1, 0).astype(BF16)

    pin, pout = iota((wide_e, lanes), 0), iota((wide_e, lanes), 1)
    pat = lax.rem(pout, 64)
    inner = lax.rem(pat, 8)
    for h in range(count_e // 2):
        chosen = jnp.zeros((wide_e, lanes), F32)
        for k in range(nb):
            for b in range(2):
                sel = jnp.where(
                    (pin == start_e + inner) & (inner < rows_e) & (pat // 8 == 2 * k + b), 1.0, 0.0
                ).astype(BF16)
                chosen = chosen + dot(se[2 * h + b, k], sel, 1, 0)
        wsel_e[h] = chosen.astype(BF16)

    for copy in load_env:
        copy.wait()
    le_all = le[...].reshape(count_e * wide_e, le.shape[2])
    pad = 64 - wide_e
    gap_rows = jnp.zeros((pad, re.shape[2]), BF16)
    re_all = cat([x for q in range(count_e) for x in (re[q], gap_rows)], 0)
    base_e = dot(le_all, re_all, 1, 1)
    low_lanes = iota((wide_e, lanes), 1) < 64
    base_h = []
    for h in range(count_e // 2):
        block = base_e[:, h * lanes : (h + 1) * lanes]
        a, b = 2 * h * wide_e, (2 * h + 1) * wide_e
        base_h.append(jnp.where(low_lanes, block[a : a + wide_e], block[b : b + wide_e]))

    def ladder(p):
        if not isinstance(p, int):
            start_pair(p + DEPTH)
        for copy in load_pair(p):
            copy.wait()
        base = dot(la[p], ra[p], 1, 1)
        tot[p] = base
        b16[p] = base.astype(BF16)

    pl.loop(0, count_a - DEPTH)(ladder)
    for p in range(count_a - DEPTH, 7):
        ladder(p)

    at_k = iota((1, lanes), 1) // rows_a
    zero = jnp.zeros((rows_a, wide_a), F32)
    rest = jnp.zeros((lanes - group, nb * wide_a), BF16)

    def couple(p):
        rows, scale = [], jnp.zeros((1, lanes), F32)
        for k in range(nb):
            nbr = blk_a[nbr_a[k, p]].astype(F32)
            rows.append(cat([nbr if i == k else zero for i in range(nb)], 1))
            scale = jnp.where(at_k == k, fock_a[k, p], scale)
        rows = cat([cat(rows, 0).astype(BF16), rest], 0)
        near[p] = (dot(overs(p), rows, 1, 1) * scale).astype(BF16)

    fill = jnp.zeros((pad, wide_e), BF16)
    lane16, row16 = iota((16, lanes), 1), iota((16, lanes), 0)
    keep16 = (lane16 < 64) == (row16 < 8)

    def couple_env(h):
        q0, q1 = 2 * h, 2 * h + 1
        parts = []
        for k in range(nb):
            both = cat([se[q0, k], fill, se[q1, k], fill], 0)
            rows = cat(
                [blk_e[nbr_e[q, k], :, :wide_e].astype(F32) for q in (q0, q1)], 0
            ).astype(BF16)
            prod = dot(rows, both, 1, 1)
            scale = jnp.where(row16 < 8, fock_e[q0, k], fock_e[q1, k])
            parts.append(jnp.where(keep16, prod * scale, 0.0))
        near = cat(halves(cat(parts, 0)), 0)
        return (base_h[h] + dot(wsel_e[h], near, 1, 0)).astype(BF16)

    arrived(blk_a.at[pl.ds(0, (npair - 1) * count_a)], blk_s, blk_r)
    arrived(blk_e.at[pl.ds(0, (npair - 1) * count_e)], ble_s, ble_r)

    for p in range(count_a):
        couple(p)
    def sums_to(c, o):
        e = o[0] * nz + o[1]
        return pltpu.make_async_remote_copy(
            src_ref=sends[c].at[peer_of(o)], dst_ref=recvs[c].at[e],
            send_sem=rs_s.at[c], recv_sem=rs_r.at[c],
            device_id={"aux": peer_of(o)}, device_id_type=MESH,
        )

    for c, (lo, hi) in enumerate(CHUNKS):
        if c == 0:
            arrived(gat0.at[pl.ds(0, naux - 1)], gat_s.at[0], gat_r.at[0])
        if c == 0:
            pass
        for p in range(lo, hi):
            if c == 0:
                amp = gat0[:, p].astype(F32).reshape(wide_a, wide_a).astype(BF16)
                x = dot(amp, b16[p], 0, 0)
            else:
                amp = gat1[:, p - lo].astype(F32).reshape(wide_a, wide_a).astype(BF16)
                x = dot(amp, b16[p], 0, 0)
            y = dot(cat([x.astype(BF16), wsel[p]], 1), cat([amp, near[p]], 1), 1, 1)
            total = (tot[p] + x + y).reshape(naux, rows_a, wide_a)
            sends[c][:, p - lo] = total.astype(BF16)
        for o in far:
            sums_to(c, o).start()
        if c == 0:
            arrived(gat1.at[pl.ds(0, naux - 1)], gat_s.at[1], gat_r.at[1])
            for p in (7, 8):
                for copy in load_pair(p):
                    copy.wait()
            both_e = cat([couple_env(h) for h in range(count_e // 2)], 0)
            srow, scol = iota((lanes, 2 * wide_e), 0), iota((lanes, 2 * wide_e), 1)
            sj, sr = srow // 8, lax.rem(srow, 8)
            si = lax.rem(sr, 4)
            spread = jnp.where(
                (scol == (sr // 4) * wide_e + rows_e * sj + si) & (si < rows_e), 1.0, 0.0
            ).astype(BF16)
            packed = dot(spread, both_e, 1, 0)
            for j in range(naux):
                send1[j, CHUNKS[1][1] - CHUNKS[1][0]] = packed[8 * j : 8 * j + 8].astype(BF16)
            for p in (7, 8):
                base = dot(la[p], ra[p], 1, 1)
                tot[p] = base
                b16[p] = base.astype(BF16)
            for p in (9,):
                for copy in load_pair(p):
                    copy.wait()
            for p in (9,):
                base = dot(la[p], ra[p], 1, 1)
                tot[p] = base
                b16[p] = base.astype(BF16)

    for c, (lo, hi) in enumerate(CHUNKS):
        arrived(recvs[c].at[pl.ds(1, naux - 1)], rs_s.at[c], rs_r.at[c])
        acc = sends[c][me].astype(F32)
        for e in range(1, naux):
            acc = acc + recvs[c][e].astype(F32)
        for p in range(lo, hi):
            out_a[p] = amp_a[p] - acc[p - lo] * rec_a[p]
        if c == 1:
            env = acc[hi - lo]
            turned = pltpu.roll(env, 64, 1)
            for q in range(count_e):
                r = 4 * (q // 2)
                block = (env if q % 2 == 0 else turned)[r : r + 4, :wide_e]
                new = amp_e[q][:4] - block * rec_e[q][:4]
                for i in range(rows_e):
                    out_e[i, q : q + 1, :] = new[i : i + 1]


def hand_over(from_a, from_e, out_a, out_e, sem):
    copies = (
        pltpu.make_async_copy(from_a, out_a, sem.at[0]),
        pltpu.make_async_copy(from_e, out_e, sem.at[1]),
    )
    for copy in copies:
        copy.start()
    for copy in copies:
        copy.wait()


def shards(
    npair, ny, nz,
    left_active, right_active, amps_active, rank_active, gap_active, energy_active,
    intersect_active, fock_active, neighbor_active,
    left_env, right_env, amps_env, rank_env, gap_env, energy_env,
    intersect_env, fock_env, neighbor_env,
):
    naux = ny * nz
    count_a, rows_a, wide_a = amps_active.shape
    count_e, rows_e, wide_e = amps_env.shape
    nb = neighbor_active.shape[1]
    vmem = pl.BlockSpec(memory_space=pltpu.VMEM)
    hbm = pl.BlockSpec(memory_space=pltpu.HBM)
    dma = pltpu.SemaphoreType.DMA
    n0 = CHUNKS[0][1] - CHUNKS[0][0]
    n1 = CHUNKS[1][1] - CHUNKS[1][0]
    small = (
        neighbor_active.T, rank_active, fock_active.T, gap_active,
        neighbor_env, rank_env, fock_env, gap_env,
        amps_active, energy_active, amps_env.transpose(1, 0, 2), energy_env,
    )
    sums = pl.pallas_call(
        functools.partial(kernel, npair, ny, nz),
        out_shape=(
            jax.ShapeDtypeStruct((count_a, rows_a, wide_a), F32),
            jax.ShapeDtypeStruct((rows_e, count_e, wide_e), F32),
        ),
        in_specs=[hbm] * 18,
        out_specs=(vmem, vmem),
        scratch_shapes=[pltpu.SMEM(x.shape, x.dtype) for x in small[:8]]
        + [pltpu.VMEM(x.shape, x.dtype) for x in small[8:]]
        + [
            pltpu.VMEM(left_active.shape, BF16),
            pltpu.VMEM(right_active.shape, BF16),
            pltpu.VMEM(intersect_active.shape, BF16),
            pltpu.VMEM(left_env.shape, BF16),
            pltpu.VMEM(right_env.shape, BF16),
            pltpu.VMEM(intersect_env.shape, BF16),
            pltpu.VMEM((naux, n0, rows_a, wide_a), BF16),
            pltpu.VMEM((naux, n1, rows_a, wide_a), BF16),
            pltpu.VMEM((npair * count_a, rows_a, wide_a), BF16),
            pltpu.VMEM((npair * count_e, 8, 128), BF16),
            pltpu.VMEM((count_a, wide_a, wide_a), F32),
            pltpu.VMEM((count_a, wide_a, wide_a), BF16),
            pltpu.VMEM((count_a, wide_a, wide_a), BF16),
            pltpu.VMEM((n1, wide_a, wide_a), BF16),
            pltpu.VMEM((n1, wide_a, wide_a), BF16),
            pltpu.VMEM((count_a, wide_a, 128), BF16),
            pltpu.VMEM((count_e // 2, wide_e, 128), BF16),
            pltpu.VMEM((count_a, rows_a, wide_a), F32),
            pltpu.VMEM((count_a, rows_a, wide_a), F32),
            pltpu.VMEM((count_e, 8, wide_e), F32),
            pltpu.VMEM((count_e, 8, wide_e), F32),
            pltpu.VMEM((naux, n0, rows_a, wide_a), BF16),
            pltpu.VMEM((naux, n1 + 1, rows_a, wide_a), BF16),
            pltpu.VMEM((naux, n0, rows_a, wide_a), BF16),
            pltpu.VMEM((naux, n1 + 1, rows_a, wide_a), BF16),
            dma((12,)), dma((count_a,)), dma((count_a,)), dma, dma, dma, dma,
            dma((2,)), dma((2,)), dma, dma, dma, dma, dma((2,)), dma((2,)),
        ],
        compiler_params=pltpu.CompilerParams(
            collective_id=0, has_side_effects=True, vmem_limit_bytes=VMEM
        ),
    )(
        *(
            pltpu.with_memory_space_constraint(x, pltpu.HBM)
            for x in small
            + (left_active, right_active, intersect_active, left_env, right_env, intersect_env)
        )
    )
    new_active, new_env = pl.pallas_call(
        hand_over,
        out_shape=(
            jax.ShapeDtypeStruct((count_a, rows_a, wide_a), F32),
            jax.ShapeDtypeStruct((rows_e, count_e, wide_e), F32),
        ),
        in_specs=[vmem, vmem],
        out_specs=(hbm, hbm),
        scratch_shapes=[dma((2,))],
        compiler_params=pltpu.CompilerParams(vmem_limit_bytes=8 * 1024 * 1024),
    )(*sums)
    return new_active, new_env.transpose(1, 0, 2)


def solution(mesh):
    ints, amps = P("pair", None, "aux"), P("pair", "aux", None)
    one, two, four = P("pair"), P("pair", None), P("pair", None, None, None)
    level = (ints, ints, amps, one, one, two, four, two, two)
    naux = mesh.shape["aux"]
    ny = next(n for n in range(int(naux**0.5), 0, -1) if naux % n == 0)
    return jax.shard_map(
        functools.partial(shards, mesh.shape["pair"], ny, naux // ny),
        mesh=mesh,
        in_specs=level + level,
        out_specs=(amps, amps),
        check_vma=False,
    )
```

```python
import functools

import jax
import jax.numpy as jnp
from jax import lax
from jax.experimental import pallas as pl
from jax.experimental.pallas import tpu as pltpu
from jax.sharding import PartitionSpec as P

MESH = pl.DeviceIdType.MESH
F32, BF16, I32 = jnp.float32, jnp.bfloat16, jnp.int32
FIRST, DEPTH = 2, 5
VMEM = 36 * 1024 * 1024
CHUNKS = ((0, 6), (6, 10))


def halves(x):
    high = x.astype(BF16)
    return high, (x - high.astype(F32)).astype(BF16)


def dot(a, b, ca, cb):
    return lax.dot_general(a, b, (((ca,), (cb,)), ((), ())), preferred_element_type=F32)


def iota(shape, dim):
    return lax.broadcasted_iota(I32, shape, dim)


def cat(parts, axis):
    return jnp.concatenate(parts, axis=axis)


def hops(d, n):
    return min(d, n - d)


def kernel(
    npair, ny, nz,
    *refs,
):
    small_hbm, refs = refs[:12], refs[12:]
    small, refs = refs[8 : 8 + 12], refs[:8] + refs[8 + 12 :]
    body(npair, ny, nz, small_hbm, small, *refs)


def body(
    npair, ny, nz, small_hbm, small,
    la_hbm, ra_hbm, sa_hbm, le_hbm, re_hbm, se_hbm,
    out_a, out_e,
    la, ra, sa, le, re, se,
    gat0, gat1, blk_a, blk_e, tot, b16, near, ampb, turn, wsel, wsel_e, amp_a, rec_a, amp_e, rec_e,
    send0, send1, recv0, recv1,
    small_sem, la_sem, ra_sem, le_sem, re_sem, sa_sem, se_sem,
    gat_s, gat_r, blk_s, blk_r, ble_s, ble_r, rs_s, rs_r,
):
    nbr_a, rank_a, fock_a, gap_a, nbr_e, rank_e, fock_e, gap_e = small[:8]
    amps_a, en_a, amps_e, en_e = small[8:]
    me, grp = lax.axis_index("aux"), lax.axis_index("pair")
    naux = ny * nz
    my, mz = me // nz, lax.rem(me, nz)
    count_a, rows_a, wide_a = amps_a.shape
    rows_e, count_e, wide_e = amps_e.shape
    nb = nbr_a.shape[0]
    lanes = wide_a
    start_a, start_e = me * rows_a, me * rows_e
    gats = (gat0, gat1)
    sends, recvs = (send0, send1), (recv0, recv1)

    far = sorted(
        ((dy, dz) for dy in range(ny) for dz in range(nz) if dy or dz),
        key=lambda o: -(hops(o[0], ny) + hops(o[1], nz)),
    )

    def peer_of(o):
        return lax.rem(my + o[0], ny) * nz + lax.rem(mz + o[1], nz)

    barrier = pltpu.get_barrier_semaphore()
    for o in far:
        pl.semaphore_signal(barrier, inc=1, device_id={"aux": peer_of(o)}, device_id_type=MESH)
    for d in range(1, npair):
        pl.semaphore_signal(
            barrier, inc=1, device_id={"pair": lax.rem(grp + d, npair)}, device_id_type=MESH
        )

    def load_pair(p):
        return (
            pltpu.make_async_copy(la_hbm.at[p], la.at[p], la_sem.at[p]),
            pltpu.make_async_copy(ra_hbm.at[p], ra.at[p], ra_sem.at[p]),
        )

    load_env = (
        pltpu.make_async_copy(le_hbm, le, le_sem),
        pltpu.make_async_copy(re_hbm, re, re_sem),
    )
    load_se = pltpu.make_async_copy(se_hbm, se, se_sem)
    load_sa = pltpu.make_async_copy(sa_hbm, sa, sa_sem)
    load_small = [
        pltpu.make_async_copy(src, dst, small_sem.at[i])
        for i, (src, dst) in enumerate(zip(small_hbm, small))
    ]
    for copy in load_small:
        copy.start()
    load_sa.start()
    load_se.start()
    for copy in load_env:
        copy.start()

    def start_pair(p):
        for copy in load_pair(p):
            copy.start()

    for p in range(FIRST):
        start_pair(p)
    for copy in load_small:
        copy.wait()

    row8, col8 = iota((rows_a, lanes), 0), iota((rows_a, lanes), 1)
    for p in range(count_a):
        inside = (start_a + row8 < rank_a[p]) & (col8 < rank_a[p])
        own = jnp.where(inside, amps_a[p].astype(F32), 0.0)
        amp_a[p] = own
        own = own.astype(BF16)
        c = 0 if p < CHUNKS[0][1] else 1
        gats[c][me, p - CHUNKS[c][0]] = own
        blk_a[grp * count_a + p] = own

    def own_env(q):
        rows = jnp.zeros((8, wide_e), F32)
        r, s = iota((8, wide_e), 0), iota((8, wide_e), 1)
        for i in range(rows_e):
            rows = jnp.where(r == i, amps_e[i, q : q + 1, :].astype(F32), rows)
        inside = (r < rows_e) & (start_e + r < rank_e[q]) & (s < rank_e[q])
        return jnp.where(inside, rows, 0.0), inside

    owns = [own_env(q) for q in range(count_e)]
    for q in range(count_e):
        at = grp * count_e + q
        blk_e[at] = jnp.zeros(blk_e.shape[1:], BF16)
        blk_e[at, :, :wide_e] = owns[q][0].astype(BF16)

    pl.semaphore_wait(barrier, naux + npair - 2)

    def to_aux(c, o):
        slot = gats[c].at[me]
        return pltpu.make_async_remote_copy(
            src_ref=slot, dst_ref=slot, send_sem=gat_s.at[c], recv_sem=gat_r.at[c],
            device_id={"aux": peer_of(o)}, device_id_type=MESH,
        )

    def arrived(ref, send, recv):
        pltpu.make_async_remote_copy(
            src_ref=ref, dst_ref=ref, send_sem=send, recv_sem=recv,
            device_id={"aux": peer_of(far[0])}, device_id_type=MESH,
        ).wait()

    def to_pair(d, block, count, s, r):
        slot = block.at[pl.ds(grp * count, count)]
        return pltpu.make_async_remote_copy(
            src_ref=slot, dst_ref=slot, send_sem=s, recv_sem=r,
            device_id={"pair": lax.rem(grp + d, npair)}, device_id_type=MESH,
        )

    for c in range(2):
        for o in far:
            to_aux(c, o).start()
        if c == 0:
            for d in range(1, npair):
                to_pair(d, blk_a, count_a, blk_s, blk_r).start()
                to_pair(d, blk_e, count_e, ble_s, ble_r).start()

    for p in range(FIRST, DEPTH):
        start_pair(p)

    for p in range(count_a):
        inside = (start_a + row8 < rank_a[p]) & (col8 < rank_a[p])
        across = jnp.broadcast_to(en_a[p : p + 1, :], (rows_a, lanes))
        down = jnp.sum(jnp.where(col8 == start_a + row8, across, 0.0), axis=1, keepdims=True)
        rec_a[p] = jnp.where(inside, 1.0 / (across + down + gap_a[p]), 0.0)
    r48, c48 = iota((8, wide_e), 0), iota((8, wide_e), 1)
    for q in range(count_e):
        across = jnp.broadcast_to(en_e[q : q + 1, :], (8, wide_e))
        down = jnp.sum(jnp.where(c48 == start_e + r48, across, 0.0), axis=1, keepdims=True)
        denom = jnp.where(r48 < rows_e, across + down + gap_e[q], 1.0)
        rec_e[q] = jnp.where(owns[q][1], 1.0 / denom, 0.0)
        amp_e[q] = owns[q][0]

    load_sa.wait()
    load_se.wait()
    group = nb * rows_a
    k_in, k_out = iota((nb * wide_a, lanes), 0), iota((nb * wide_a, lanes), 1)
    k_at = lax.rem(k_out, group)
    source = (k_at // rows_a) * wide_a + start_a + lax.rem(k_at, rows_a)
    pick = jnp.where((k_in == source) & (k_out < group), 1.0, 0.0).astype(BF16)

    def overs(p):
        return cat([sa[p, k] for k in range(nb)], 1)

    for p in range(count_a):
        wsel[p] = dot(overs(p), pick, 1, 0).astype(BF16)

    pin, pout = iota((wide_e, lanes), 0), iota((wide_e, lanes), 1)
    pat = lax.rem(pout, 64)
    inner = lax.rem(pat, 8)
    for h in range(count_e // 2):
        chosen = jnp.zeros((wide_e, lanes), F32)
        for k in range(nb):
            for b in range(2):
                sel = jnp.where(
                    (pin == start_e + inner) & (inner < rows_e) & (pat // 8 == 2 * k + b), 1.0, 0.0
                ).astype(BF16)
                chosen = chosen + dot(se[2 * h + b, k], sel, 1, 0)
        wsel_e[h] = chosen.astype(BF16)

    def ladder(p):
        if not isinstance(p, int):
            start_pair(p + DEPTH)
        for copy in load_pair(p):
            copy.wait()
        base = dot(la[p], ra[p], 1, 1)
        tot[p] = base
        b16[p] = base.astype(BF16)

    pl.loop(0, 2)(ladder)
    for copy in load_env:
        copy.wait()
    le_all = le[...].reshape(count_e * wide_e, le.shape[2])
    pad = 64 - wide_e
    gap_rows = jnp.zeros((pad, re.shape[2]), BF16)
    re_all = cat([x for q in range(count_e) for x in (re[q], gap_rows)], 0)
    base_e = dot(le_all, re_all, 1, 1)
    low_lanes = iota((wide_e, lanes), 1) < 64
    base_h = []
    for h in range(count_e // 2):
        block = base_e[:, h * lanes : (h + 1) * lanes]
        a, b = 2 * h * wide_e, (2 * h + 1) * wide_e
        base_h.append(jnp.where(low_lanes, block[a : a + wide_e], block[b : b + wide_e]))

    pl.loop(2, count_a - DEPTH)(ladder)
    for p in range(count_a - DEPTH, 7):
        ladder(p)

    at_k = iota((1, lanes), 1) // rows_a
    zero = jnp.zeros((rows_a, wide_a), F32)
    rest = jnp.zeros((lanes - group, nb * wide_a), BF16)

    def couple(p):
        rows, scale = [], jnp.zeros((1, lanes), F32)
        for k in range(nb):
            nbr = blk_a[nbr_a[k, p]].astype(F32)
            rows.append(cat([nbr if i == k else zero for i in range(nb)], 1))
            scale = jnp.where(at_k == k, fock_a[k, p], scale)
        rows = cat([cat(rows, 0).astype(BF16), rest], 0)
        near[p] = (dot(overs(p), rows, 1, 1) * scale).astype(BF16)

    fill = jnp.zeros((pad, wide_e), BF16)
    lane16, row16 = iota((16, lanes), 1), iota((16, lanes), 0)
    keep16 = (lane16 < 64) == (row16 < 8)

    def couple_env(h):
        q0, q1 = 2 * h, 2 * h + 1
        parts = []
        for k in range(nb):
            both = cat([se[q0, k], fill, se[q1, k], fill], 0)
            rows = cat(
                [blk_e[nbr_e[q, k], :, :wide_e].astype(F32) for q in (q0, q1)], 0
            ).astype(BF16)
            prod = dot(rows, both, 1, 1)
            scale = jnp.where(row16 < 8, fock_e[q0, k], fock_e[q1, k])
            parts.append(jnp.where(keep16, prod * scale, 0.0))
        near = cat(halves(cat(parts, 0)), 0)
        return (base_h[h] + dot(wsel_e[h], near, 1, 0)).astype(BF16)

    arrived(blk_a.at[pl.ds(0, (npair - 1) * count_a)], blk_s, blk_r)
    arrived(blk_e.at[pl.ds(0, (npair - 1) * count_e)], ble_s, ble_r)

    for p in range(count_a):
        couple(p)
    def sums_to(c, o):
        e = o[0] * nz + o[1]
        return pltpu.make_async_remote_copy(
            src_ref=sends[c].at[peer_of(o)], dst_ref=recvs[c].at[e],
            send_sem=rs_s.at[c], recv_sem=rs_r.at[c],
            device_id={"aux": peer_of(o)}, device_id_type=MESH,
        )

    for c, (lo, hi) in enumerate(CHUNKS):
        if c == 0:
            arrived(gat0.at[pl.ds(0, naux - 1)], gat_s.at[0], gat_r.at[0])
        if c == 0:
            pass
        for p in range(lo, hi):
            if c == 0:
                amp = gat0[:, p].astype(F32).reshape(wide_a, wide_a).astype(BF16)
                x = dot(amp, b16[p], 0, 0)
            else:
                amp = gat1[:, p - lo].astype(F32).reshape(wide_a, wide_a).astype(BF16)
                x = dot(amp, b16[p], 0, 0)
            y = dot(cat([x.astype(BF16), wsel[p]], 1), cat([amp, near[p]], 1), 1, 1)
            total = (tot[p] + x + y).reshape(naux, rows_a, wide_a)
            sends[c][:, p - lo] = total.astype(BF16)
        for o in far:
            sums_to(c, o).start()
        if c == 0:
            arrived(gat1.at[pl.ds(0, naux - 1)], gat_s.at[1], gat_r.at[1])
            for p in (7, 8):
                for copy in load_pair(p):
                    copy.wait()
            both_e = cat([couple_env(h) for h in range(count_e // 2)], 0)
            srow, scol = iota((lanes, 2 * wide_e), 0), iota((lanes, 2 * wide_e), 1)
            sj, sr = srow // 8, lax.rem(srow, 8)
            si = lax.rem(sr, 4)
            spread = jnp.where(
                (scol == (sr // 4) * wide_e + rows_e * sj + si) & (si < rows_e), 1.0, 0.0
            ).astype(BF16)
            packed = dot(spread, both_e, 1, 0)
            for j in range(naux):
                send1[j, CHUNKS[1][1] - CHUNKS[1][0]] = packed[8 * j : 8 * j + 8].astype(BF16)
            for p in (7, 8):
                base = dot(la[p], ra[p], 1, 1)
                tot[p] = base
                b16[p] = base.astype(BF16)
            for p in (9,):
                for copy in load_pair(p):
                    copy.wait()
            for p in (9,):
                base = dot(la[p], ra[p], 1, 1)
                tot[p] = base
                b16[p] = base.astype(BF16)

    for c, (lo, hi) in enumerate(CHUNKS):
        arrived(recvs[c].at[pl.ds(1, naux - 1)], rs_s.at[c], rs_r.at[c])
        acc = sends[c][me].astype(F32)
        for e in range(1, naux):
            acc = acc + recvs[c][e].astype(F32)
        for p in range(lo, hi):
            out_a[p] = amp_a[p] - acc[p - lo] * rec_a[p]
        if c == 1:
            env = acc[hi - lo]
            turned = pltpu.roll(env, 64, 1)
            for q in range(count_e):
                r = 4 * (q // 2)
                block = (env if q % 2 == 0 else turned)[r : r + 4, :wide_e]
                new = amp_e[q][:4] - block * rec_e[q][:4]
                for i in range(rows_e):
                    out_e[i, q : q + 1, :] = new[i : i + 1]


def hand_over(from_a, from_e, out_a, out_e, sem):
    copies = (
        pltpu.make_async_copy(from_a, out_a, sem.at[0]),
        pltpu.make_async_copy(from_e, out_e, sem.at[1]),
    )
    for copy in copies:
        copy.start()
    for copy in copies:
        copy.wait()


def shards(
    npair, ny, nz,
    left_active, right_active, amps_active, rank_active, gap_active, energy_active,
    intersect_active, fock_active, neighbor_active,
    left_env, right_env, amps_env, rank_env, gap_env, energy_env,
    intersect_env, fock_env, neighbor_env,
):
    naux = ny * nz
    count_a, rows_a, wide_a = amps_active.shape
    count_e, rows_e, wide_e = amps_env.shape
    nb = neighbor_active.shape[1]
    vmem = pl.BlockSpec(memory_space=pltpu.VMEM)
    hbm = pl.BlockSpec(memory_space=pltpu.HBM)
    dma = pltpu.SemaphoreType.DMA
    n0 = CHUNKS[0][1] - CHUNKS[0][0]
    n1 = CHUNKS[1][1] - CHUNKS[1][0]
    small = (
        neighbor_active.T, rank_active, fock_active.T, gap_active,
        neighbor_env, rank_env, fock_env, gap_env,
        amps_active, energy_active, amps_env.transpose(1, 0, 2), energy_env,
    )
    sums = pl.pallas_call(
        functools.partial(kernel, npair, ny, nz),
        out_shape=(
            jax.ShapeDtypeStruct((count_a, rows_a, wide_a), F32),
            jax.ShapeDtypeStruct((rows_e, count_e, wide_e), F32),
        ),
        in_specs=[hbm] * 18,
        out_specs=(vmem, vmem),
        scratch_shapes=[pltpu.SMEM(x.shape, x.dtype) for x in small[:8]]
        + [pltpu.VMEM(x.shape, x.dtype) for x in small[8:]]
        + [
            pltpu.VMEM(left_active.shape, BF16),
            pltpu.VMEM(right_active.shape, BF16),
            pltpu.VMEM(intersect_active.shape, BF16),
            pltpu.VMEM(left_env.shape, BF16),
            pltpu.VMEM(right_env.shape, BF16),
            pltpu.VMEM(intersect_env.shape, BF16),
            pltpu.VMEM((naux, n0, rows_a, wide_a), BF16),
            pltpu.VMEM((naux, n1, rows_a, wide_a), BF16),
            pltpu.VMEM((npair * count_a, rows_a, wide_a), BF16),
            pltpu.VMEM((npair * count_e, 8, 128), BF16),
            pltpu.VMEM((count_a, wide_a, wide_a), F32),
            pltpu.VMEM((count_a, wide_a, wide_a), BF16),
            pltpu.VMEM((count_a, wide_a, wide_a), BF16),
            pltpu.VMEM((n1, wide_a, wide_a), BF16),
            pltpu.VMEM((n1, wide_a, wide_a), BF16),
            pltpu.VMEM((count_a, wide_a, 128), BF16),
            pltpu.VMEM((count_e // 2, wide_e, 128), BF16),
            pltpu.VMEM((count_a, rows_a, wide_a), F32),
            pltpu.VMEM((count_a, rows_a, wide_a), F32),
            pltpu.VMEM((count_e, 8, wide_e), F32),
            pltpu.VMEM((count_e, 8, wide_e), F32),
            pltpu.VMEM((naux, n0, rows_a, wide_a), BF16),
            pltpu.VMEM((naux, n1 + 1, rows_a, wide_a), BF16),
            pltpu.VMEM((naux, n0, rows_a, wide_a), BF16),
            pltpu.VMEM((naux, n1 + 1, rows_a, wide_a), BF16),
            dma((12,)), dma((count_a,)), dma((count_a,)), dma, dma, dma, dma,
            dma((2,)), dma((2,)), dma, dma, dma, dma, dma((2,)), dma((2,)),
        ],
        compiler_params=pltpu.CompilerParams(
            collective_id=0, has_side_effects=True, vmem_limit_bytes=VMEM
        ),
    )(
        *(
            pltpu.with_memory_space_constraint(x, pltpu.HBM)
            for x in small
            + (left_active, right_active, intersect_active, left_env, right_env, intersect_env)
        )
    )
    new_active, new_env = pl.pallas_call(
        hand_over,
        out_shape=(
            jax.ShapeDtypeStruct((count_a, rows_a, wide_a), F32),
            jax.ShapeDtypeStruct((rows_e, count_e, wide_e), F32),
        ),
        in_specs=[vmem, vmem],
        out_specs=(hbm, hbm),
        scratch_shapes=[dma((2,))],
        compiler_params=pltpu.CompilerParams(vmem_limit_bytes=8 * 1024 * 1024),
    )(*sums)
    return new_active, new_env.transpose(1, 0, 2)


def solution(mesh):
    ints, amps = P("pair", None, "aux"), P("pair", "aux", None)
    one, two, four = P("pair"), P("pair", None), P("pair", None, None, None)
    level = (ints, ints, amps, one, one, two, four, two, two)
    naux = mesh.shape["aux"]
    ny = next(n for n in range(int(naux**0.5), 0, -1) if naux % n == 0)
    return jax.shard_map(
        functools.partial(shards, mesh.shape["pair"], ny, naux // ny),
        mesh=mesh,
        in_specs=level + level,
        out_specs=(amps, amps),
        check_vma=False,
    )
```
